256 devices in a mesh: dp: 32 (over z, y_lo, core), chan: 8 (over y_hi, x).
Axes of the slice: x: 4, y: 4 (y_hi: 2, y_lo: 2; y = y_hi * 2 + y_lo), z: 8, core: 2. Of those that a mesh axis runs over, the one named last changes fastest.
Arguments:
- inputs: bfloat16 [1536, 196, 1024], P('dp', None, 'chan'), may hold values from -6 to 6
- norm_gain: float32 [1024], P('chan'), may hold values from 0.5 to 1.5
- norm_bias: float32 [1024], P('chan'), may hold values from -3 to 3
- w_first: bfloat16 [512, 196], replicated, may hold values from -0.4375 to 0.4375
- b_first: float32 [512], replicated, may hold values from -3 to 3
- w_second: bfloat16 [196, 512], replicated, may hold values from -0.25 to 0.25
- upstream: bfloat16 [1536, 196, 1024], P('dp', None, 'chan'), may hold values from -6 to 6
Outputs:
- grad_input: bfloat16 [1536, 196, 1024], P('dp', None, 'chan')
- grad_first: float32 [512, 196], P('dp')
- grad_second: float32 [196, 512], P(None, 'dp')
- grad_bias_first: float32 [512], P('dp')
- grad_gain: float32 [1024], P('chan')
- grad_shift: float32 [1024], P('chan')
The draws below stay inside these ranges and needn't reach their ends.
All inputs are finite; a program needn't handle non-finite values.
Results may differ from the reference program's by a relative error of at most 0.0056.
Values sent between devices are 32-bit elements; how exact they have to be, the bound alone decides.
A program may use at most 64 MiB of HBM per device.

```python
import jax
import jax.numpy as jnp
from jax import lax

D = 1024
PATCHES = 196
TOKEN_HIDDEN = 512
B_DEV = 48
BATCH = 1536
N_DP = 32


def shard_levels(key, shape, pieces, low, high):
    factor_of = 1.0
    for axis_at, shards_of in pieces:
        heights = jax.random.uniform(jax.random.fold_in(jax.random.fold_in(key, 6), axis_at), (shards_of,), jnp.float32, low / len(pieces), high / len(pieces))
        factor_of = factor_of * jnp.repeat(jnp.exp(heights), shape[axis_at] // shards_of).reshape((-1,) + (1,) * (len(shape) - 1 - axis_at))
    return factor_of


def centred(rng, shape, spread, limit, shards=(), held_as=jnp.bfloat16):
    level = shard_levels(rng, shape, shards, -0.22, 0.18) if shards else 1.0
    array = jax.random.normal(rng, shape, jnp.float32) * spread * level
    return jnp.minimum(jnp.maximum(array, -limit), limit).astype(held_as)


def setup_inputs(seed: int = 0) -> dict:
    arg_keys = jax.random.split(jax.random.key(seed), 8)
    inputs = centred(arg_keys[0], (BATCH, PATCHES, D), 1.0, 6.0, ((0, 32), (2, 8)))
    norm_gain = jnp.clip(1.0 + 0.1 * jax.random.normal(arg_keys[1], (D,), jnp.float32), 0.5, 1.5)
    norm_bias = centred(arg_keys[2], (D,), 0.5, 3.0, ((0, 8),), jnp.float32)
    w_first = centred(arg_keys[3], (TOKEN_HIDDEN, PATCHES), PATCHES ** -0.5, 0.4375)
    b_first = centred(arg_keys[4], (TOKEN_HIDDEN,), 0.5, 3.0, (), jnp.float32)
    w_second = centred(arg_keys[5], (PATCHES, TOKEN_HIDDEN), TOKEN_HIDDEN ** -0.5, 0.25)
    upstream = centred(arg_keys[6], (BATCH, PATCHES, D), 1.0, 6.0, ((0, 32), (2, 8)))
    return dict(inputs=inputs, norm_gain=norm_gain, norm_bias=norm_bias, w_first=w_first, b_first=b_first, w_second=w_second, upstream=upstream)


epsilon = 1e-06

def block_pass(values_in, upstream, norm_gain, norm_bias, w_first, b_first, w_second):
    values = values_in.astype(jnp.float32)
    row_mean = lax.optimization_barrier(jnp.mean(values, axis=-1, keepdims=True))
    centered = values - row_mean
    row_var = lax.optimization_barrier(jnp.mean(centered * centered, axis=-1, keepdims=True))
    inv_std = lax.rsqrt(row_var + epsilon)
    normed = centered * inv_std
    mixed_in = (normed * norm_gain + norm_bias).astype(jnp.bfloat16)
    pre_act = jnp.einsum('kp,bpc->bkc', w_first.astype(jnp.float32), mixed_in.astype(jnp.float32)) + b_first[None, :, None]
    gauss_cdf = 0.5 * (1.0 + lax.erf(pre_act * 0.7071067811865476))
    gauss_pdf = jnp.exp(-0.5 * pre_act * pre_act) * 0.3989422804014327
    activated = (pre_act * gauss_cdf).astype(jnp.bfloat16)
    upper = upstream.astype(jnp.float32)
    grad_act = jnp.einsum('pk,bpc->bkc', w_second.astype(jnp.float32), upper)
    grad_pre = (grad_act * (gauss_cdf + pre_act * gauss_pdf)).astype(jnp.bfloat16)
    pre_f = grad_pre.astype(jnp.float32)
    second_t = jnp.einsum('bkc,bpc->kp', activated.astype(jnp.float32), upper)
    first_w = jnp.einsum('bkc,bpc->kp', pre_f, mixed_in.astype(jnp.float32))
    first_b = lax.optimization_barrier(jnp.sum(pre_f, axis=(0, 2)))
    grad_mixed = jnp.einsum('kp,bkc->bpc', w_first.astype(jnp.float32), pre_f)
    gain_part = lax.optimization_barrier(jnp.sum(grad_mixed * normed, axis=(0, 1)))
    shift_part = lax.optimization_barrier(jnp.sum(grad_mixed, axis=(0, 1)))
    grad_normed = grad_mixed * norm_gain
    first_sum = lax.optimization_barrier(jnp.sum(grad_normed, axis=-1, keepdims=True))
    second_sum = lax.optimization_barrier(jnp.sum(grad_normed * normed, axis=-1, keepdims=True))
    grad_input = (upper + inv_std * (grad_normed - first_sum / D - normed * second_sum / D)).astype(jnp.bfloat16)
    return (grad_input, first_w, second_t, first_b, gain_part, shift_part)

def reference(inputs, norm_gain, norm_bias, w_first, b_first, w_second, upstream):
    blocks_in = inputs.reshape(N_DP, B_DEV, PATCHES, D)
    blocks_up = upstream.reshape(N_DP, B_DEV, PATCHES, D)

    def step(carry, pair):
        grad_in, first_w, second_t, first_b, gain_part, shift_part = block_pass(pair[0], pair[1], norm_gain, norm_bias, w_first, b_first, w_second)
        carry = (carry[0] + first_w, carry[1] + second_t, carry[2] + first_b, carry[3] + gain_part, carry[4] + shift_part)
        return (carry, grad_in)
    init = (jnp.zeros((TOKEN_HIDDEN, PATCHES), jnp.float32), jnp.zeros((TOKEN_HIDDEN, PATCHES), jnp.float32), jnp.zeros((TOKEN_HIDDEN,), jnp.float32), jnp.zeros((D,), jnp.float32), jnp.zeros((D,), jnp.float32))
    totals, grads = lax.scan(step, init, (blocks_in, blocks_up))
    scale = 1.0 / BATCH
    grad_input = grads.reshape(BATCH, PATCHES, D)
    return (grad_input, totals[0] * scale, (totals[1] * scale).T, totals[2] * scale, totals[3] * scale, totals[4] * scale)
```

```python
import functools

import jax
import jax.numpy as jnp
from jax import lax
from jax.experimental import pallas as pl
from jax.experimental.pallas import tpu as pltpu
from jax.sharding import PartitionSpec as P

EPS = 1e-06
NB = 16
PP = 208
LANES = 128
F32 = jnp.float32
BF16 = jnp.bfloat16


def contract_lanes(a, b):
    return lax.dot_general(a, b, (((1,), (1,)), ((), ())), preferred_element_type=F32)


def kernel(
    n_dp, n_chan, patches, width, scale,
    x_hbm, u_hbm, gain_ref, bias_ref, w1a_ref, w1t_ref, w2t_ref,
    out_ref, first_ref, second_ref, vec_ref,
    x_v, u_v, mx, up, ga, gp, act, normed_n, gm_n, tmp, inv_d, acc,
    a_send, a_recv, b_send, b_recv, p0_recv, csum, c1_recv, c1_sum, c2_recv, d_send, d_recv,
    load_sem, as_sem, ar_sem, bs_sem, br_sem, p0s_sem, p0r_sem, c1s_sem, c1r_sem, c2s_sem, c2r_sem, ds_sem, dr_sem,
):
    me_d = lax.axis_index("dp")
    me_c = lax.axis_index("chan")
    core = lax.rem(me_d, 2)
    me_g = lax.div(me_d, 2)
    groups = n_dp // 2
    chunks = x_v.shape[1] // NB
    hid = w1a_ref.shape[0]
    half = hid // 2
    tiles = NB // 2
    span = NB * LANES

    def chan_peer(j):
        return lax.rem(me_c + j, n_chan)

    def dp_peer(j):
        return lax.rem(me_d + j, n_dp)

    def remote(src, dst, ssem, rsem, dp, chan):
        return pltpu.make_async_remote_copy(
            src_ref=src, dst_ref=dst, send_sem=ssem, recv_sem=rsem,
            device_id={"dp": dp, "chan": chan}, device_id_type=pl.DeviceIdType.MESH,
        )

    barrier = pltpu.get_barrier_semaphore()
    for j in range(1, n_chan):
        pl.semaphore_signal(barrier, inc=1, device_id={"dp": me_d, "chan": chan_peer(j)}, device_id_type=pl.DeviceIdType.MESH)
    for j in range(1, n_dp):
        pl.semaphore_signal(barrier, inc=1, device_id={"dp": dp_peer(j), "chan": me_c}, device_id_type=pl.DeviceIdType.MESH)

    def load(which, src, dst, ch):
        rows = pl.ds(ch * NB, NB)
        return pltpu.make_async_copy(src.at[:, rows, :], dst.at[:, rows, :], load_sem.at[which, ch])

    for ch in range(chunks):
        load(0, x_hbm, x_v, ch).start()
    for ch in range(chunks):
        load(1, u_hbm, u_v, ch).start()

    lane = lax.broadcasted_iota(jnp.int32, (NB, LANES), 1)

    def lane_tiles(body, init):
        out = []
        for lo in range(0, patches, LANES):
            count = min(LANES, patches - lo)

            def step(q, carry, lo=lo):
                for i in range(4):
                    carry = body(lo + q * 4 + i, q * 4 + i, carry)
                return carry

            out.append(lax.fori_loop(0, count // 4, step, init))
        return out

    zero = jnp.zeros((NB, LANES), F32)

    for ch in range(chunks):
        load(0, x_hbm, x_v, ch).wait()

        def stat(p, at, carry, ch=ch):
            s, q = carry
            v = x_v[p, pl.ds(ch * NB, NB), :].astype(F32)
            hit = lane == at
            s = jnp.where(hit, jnp.sum(v, axis=-1, keepdims=True), s)
            q = jnp.where(hit, jnp.sum(v * v, axis=-1, keepdims=True), q)
            return s, q

        for t, (s, q) in enumerate(lane_tiles(stat, (zero, zero))):
            a_send[ch, :, pl.ds(t * LANES, LANES)] = s
            a_send[ch, :, pl.ds((2 + t) * LANES, LANES)] = q
        if ch == 0:
            pl.semaphore_wait(barrier, n_chan - 1 + n_dp - 1)
        for j in range(1, n_chan):
            remote(a_send.at[ch], a_recv.at[ch, j], as_sem.at[ch, j], ar_sem.at[ch, j], me_d, chan_peer(j)).start()

    def regroup(g, ch, dst, value, fill):
        for i in range(16):
            tmp[pl.ds(i * NB, NB), :] = value(i)
        for b in range(NB):
            v = tmp[pl.ds(b, 16, stride=NB), :]
            if fill is not None:
                v = fill(v)
            at = pl.multiple_of(ch * span + b * LANES, LANES)
            rows = pl.ds(pl.multiple_of(g * 16, 16), 16)
            dst[rows, pl.ds(at, LANES)] = v.astype(BF16)

    full = patches // 16
    rest = patches - full * 16
    sub = lax.broadcasted_iota(jnp.int32, (16, LANES), 0)

    for ch in range(chunks):
        load(1, u_hbm, u_v, ch).wait()

        def up_group(g, _, ch=ch):
            regroup(g, ch, up, lambda i: u_v[g * 16 + i, pl.ds(ch * NB, NB), :].astype(F32), None)
            return 0

        lax.fori_loop(0, full, up_group, 0)
        regroup(
            full, ch, up,
            lambda i, ch=ch: u_v[full * 16 + min(i, rest - 1), pl.ds(ch * NB, NB), :].astype(F32),
            lambda v: jnp.where(sub < rest, v, 0.0),
        )

    def ga_tile(n, _):
        at = pl.ds(pl.multiple_of(n * 256, 256), 256)
        ga[:, at] = jnp.dot(w2t_ref[...], up[:, at], preferred_element_type=F32)
        return 0

    lax.fori_loop(0, chunks * tiles, ga_tile, 0)

    gain = gain_ref[...]
    bias = bias_ref[...]

    def wait_a(ch):
        total = a_send[ch]
        for j in range(1, n_chan):
            remote(a_send.at[ch], a_recv.at[ch, j], as_sem.at[ch, j], ar_sem.at[ch, j], me_d, chan_peer(j)).wait_recv()
            total = total + a_recv[ch, j]
        mean = total[:, : 2 * LANES] / width
        var = total[:, 2 * LANES :] / width - mean * mean
        return mean, lax.rsqrt(var + EPS)

    def column(value, i):
        return jnp.broadcast_to(value[:, i : i + 1], (NB, LANES))

    def normalise(ch):
        mean, inv = wait_a(ch)
        inv_d[ch] = inv
        mean_ref, inv_ref = a_send.at[ch], inv_d.at[ch]

        def one(g, mean16, inv16, count):
            def value(i):
                i = min(i, count - 1)
                p = g * 16 + i
                v = x_v[p, pl.ds(ch * NB, NB), :].astype(F32)
                normed = (v - column(mean16, i)) * column(inv16, i)
                normed_n[ch, pl.ds(pl.multiple_of(p * NB, NB), NB), :] = normed
                return normed * gain + bias

            fill = None
            if count < 16:
                fill = lambda v: jnp.where(sub < rest, v, jnp.where(sub < rest + 3, 1.0, 0.0))
            regroup(g, ch, mx, value, fill)

        for t in range(2):
            m_t = mean[:, t * LANES : (t + 1) * LANES]
            i_t = inv[:, t * LANES : (t + 1) * LANES]
            per = LANES // 16

            def group(g, carry, t=t):
                m, v = carry
                one(t * per + g, m, v, 16)
                return pltpu.roll(m, LANES - 16, 1), pltpu.roll(v, LANES - 16, 1)

            m_t, i_t = lax.fori_loop(0, min(per, full - t * per), group, (m_t, i_t))
        one(full, m_t, i_t, rest)

    def hidden(h, ch):
        rows = pl.ds(h * half, half)

        def tile(n, _):
            at = pl.ds(pl.multiple_of(ch * span + n * 256, 256), 256)
            pre = jnp.dot(w1a_ref[rows, :], mx[:, at], preferred_element_type=F32)
            t = pre * 0.7071067811865476
            cdf = 0.5 * lax.erf(t) + 0.5
            act[:, pl.ds(pl.multiple_of(n * 256, 256), 256)] = (pre * cdf).astype(BF16)
            slope = cdf + (t * 0.5641895835477563) * jnp.exp(-(t * t))
            gp[rows, at] = (ga[rows, at] * slope).astype(BF16)
            return 0

        lax.fori_loop(0, tiles, tile, 0)
        at = pl.ds(ch * span, span)
        first = contract_lanes(gp[rows, at], mx[:, at]).reshape(groups, 2, -1, PP)
        second = contract_lanes(act[...], up[:, at]).reshape(groups, 2, -1, PP)
        if ch:
            first = first + acc[h, :, :, :, pl.ds(0, PP)]
            second = second + acc[h, :, :, :, pl.ds(256, PP)]
        acc[h, :, :, :, pl.ds(0, PP)] = first
        acc[h, :, :, :, pl.ds(256, PP)] = second

    def p0(h):
        return remote(acc.at[h, :, 1 - core], p0_recv.at[h], p0s_sem.at[h], p0r_sem.at[h], me_d + 1 - 2 * core, me_c)

    def c1(h, j):
        g = lax.rem(me_g + j, groups)
        return remote(csum.at[h, g], c1_recv.at[h, me_g], c1s_sem.at[h, j], c1r_sem.at[h, me_g], 2 * g + core, me_c)

    def c1_arrival(h, j):
        g = lax.rem(me_g + j, groups)
        return remote(csum.at[h, g], c1_recv.at[h, g], c1s_sem.at[h, j], c1r_sem.at[h, g], 2 * g + core, me_c)

    def c2(h, j):
        return remote(c1_sum.at[h], c2_recv.at[h, me_c], c2s_sem.at[h, j], c2r_sem.at[h, me_c], me_d, chan_peer(j))

    def c2_arrival(h, j):
        c = chan_peer(j)
        return remote(c1_sum.at[h], c2_recv.at[h, c], c2s_sem.at[h, j], c2r_sem.at[h, c], me_d, c)

    def pair_done(h):
        p0(h).wait()
        csum[h] = acc[h, :, core] + p0_recv[h]
        for j in range(1, groups):
            c1(h, j).start()

    def group_done(h):
        c1_recv[h, me_g] = csum[h, me_g]
        for j in range(1, groups):
            c1_arrival(h, j).wait_recv()
        total = c1_recv[h, 0]
        for g in range(1, groups):
            total = total + c1_recv[h, g]
        c1_sum[h] = total
        c2_recv[h, me_c] = total
        for j in range(1, n_chan):
            c2(h, j).start()

    def all_done(h):
        for j in range(1, n_chan):
            c2_arrival(h, j).wait_recv()
        total = c2_recv[h, 0]
        for c in range(1, n_chan):
            total = total + c2_recv[h, c]
        total = total * scale
        first_ref[pl.ds(h * 8, 8), :] = total[:, :256]
        second_ref[pl.ds(h * 8, 8), :] = total[:, 256 : 256 + patches]

    for ch in range(chunks):
        normalise(ch)
        hidden(0, ch)
    p0(0).start()
    for ch in range(chunks):
        hidden(1, ch)
        if ch == 0:
            pair_done(0)
    p0(1).start()

    grads = (zero, zero)
    for ch in range(chunks):

        def back(n, _, ch=ch):
            at = pl.ds(pl.multiple_of(ch * span + n * 256, 256), 256)
            gm = jnp.dot(w1t_ref[...], gp[:, at], preferred_element_type=F32)
            for i in range(2):
                gm_n[ch, pl.ds(n * 2 + i, patches, stride=NB), :] = gm[:, i * LANES : (i + 1) * LANES]
            return 0

        lax.fori_loop(0, tiles, back, 0)

        def sums(p, at, carry, ch=ch):
            f, s, dg, ds = carry
            rows = pl.ds(pl.multiple_of(p * NB, NB), NB)
            gm = gm_n[ch, rows, :]
            normed = normed_n[ch, rows, :]
            both = gm * normed
            hit = lane == at
            f = jnp.where(hit, jnp.sum(gm * gain, axis=-1, keepdims=True), f)
            s = jnp.where(hit, jnp.sum(both * gain, axis=-1, keepdims=True), s)
            return f, s, dg + both, ds + gm

        for t, (f, s, dg, ds) in enumerate(lane_tiles(sums, (zero, zero, zero, zero))):
            b_send[ch, :, pl.ds(t * LANES, LANES)] = f
            b_send[ch, :, pl.ds((2 + t) * LANES, LANES)] = s
            grads = (grads[0] + dg, grads[1] + ds)
        for j in range(1, n_chan):
            remote(b_send.at[ch], b_recv.at[ch, j], bs_sem.at[ch, j], br_sem.at[ch, j], me_d, chan_peer(j)).start()
        if ch == 0:
            pair_done(1)

    mine = jnp.concatenate([jnp.sum(v, axis=0, keepdims=True) for v in grads], axis=0)
    d_send[...] = mine
    d_recv[me_d] = mine
    for j in range(1, n_dp):
        remote(d_send, d_recv.at[me_d], ds_sem.at[j], dr_sem.at[me_d], dp_peer(j), me_c).start()
    group_done(0)

    for ch in range(chunks):
        total = b_send[ch]
        for j in range(1, n_chan):
            remote(b_send.at[ch], b_recv.at[ch, j], bs_sem.at[ch, j], br_sem.at[ch, j], me_d, chan_peer(j)).wait_recv()
            total = total + b_recv[ch, j]
        inv = inv_d[ch]
        f = total[:, : 2 * LANES] * inv / width
        s = total[:, 2 * LANES :] * inv / width

        for t in range(2):
            lo = t * LANES
            count = min(LANES, patches - lo)
            cut = slice(lo, lo + LANES)

            def finish(q, carry, ch=ch, lo=lo):
                i_t, f_t, s_t = carry
                for i in range(4):
                    p = lo + q * 4 + i
                    rows = pl.ds(pl.multiple_of(p * NB, NB), NB)
                    bs = pl.ds(ch * NB, NB)
                    gn = gm_n[ch, rows, :] * gain
                    v = u_v[p, bs, :].astype(F32) + column(i_t, i) * gn - column(f_t, i) - column(s_t, i) * normed_n[ch, rows, :]
                    out_ref[p, bs, :] = v.astype(BF16)
                return tuple(pltpu.roll(c, LANES - 4, 1) for c in carry)

            lax.fori_loop(0, count // 4, finish, (inv[:, cut], f[:, cut], s[:, cut]))

    group_done(1)
    all_done(0)
    for j in range(1, n_dp):
        d = dp_peer(j)
        remote(d_send, d_recv.at[d], ds_sem.at[j], dr_sem.at[d], d, me_c).wait_recv()
    vec = d_recv[0]
    for d in range(1, n_dp):
        vec = vec + d_recv[d]
    vec_ref[...] = vec * scale
    all_done(1)

    for ch in range(chunks):
        for j in range(1, n_chan):
            remote(a_send.at[ch], a_recv.at[ch, j], as_sem.at[ch, j], ar_sem.at[ch, j], me_d, chan_peer(j)).wait_send()
            remote(b_send.at[ch], b_recv.at[ch, j], bs_sem.at[ch, j], br_sem.at[ch, j], me_d, chan_peer(j)).wait_send()
    for h in range(2):
        for j in range(1, groups):
            c1(h, j).wait_send()
        for j in range(1, n_chan):
            c2(h, j).wait_send()
    for j in range(1, n_dp):
        remote(d_send, d_recv.at[me_d], ds_sem.at[j], dr_sem.at[me_d], dp_peer(j), me_c).wait_send()


def by_owner(w, groups):
    hid, n = w.shape
    r = hid // (groups * 4)
    return w.reshape(groups, 2, 2, r, n).transpose(2, 0, 1, 3, 4).reshape(hid, n)


def per_device(n_dp, n_chan, inputs, norm_gain, norm_bias, w_first, b_first, w_second, upstream):
    images, patches, local = inputs.shape
    hid = w_first.shape[0]
    groups = n_dp // 2
    chunks = images // NB
    width = float(local * n_chan)
    scale = 1.0 / (images * n_dp)
    hi = lax.reduce_precision(b_first, 8, 7)
    mid = lax.reduce_precision(b_first - hi, 8, 7)
    low = b_first - hi - mid
    cols = jnp.stack([hi, mid, low], axis=1).astype(BF16)
    w1 = by_owner(w_first, groups)
    pad = jnp.zeros((hid, PP - patches - 3), BF16)
    w1a = jnp.concatenate([w1, by_owner(cols, groups), pad], axis=1)
    w1t = w1.T
    w2t = jnp.pad(by_owner(w_second.T, groups), ((0, 0), (0, PP - patches)))
    rows = hid // (groups * 4)
    stat = (chunks, NB, 4 * LANES)
    vmem = pl.BlockSpec(memory_space=pltpu.VMEM)
    hbm = pl.BlockSpec(memory_space=pl.ANY)
    dma = pltpu.SemaphoreType.DMA
    out, first, second, vec = pl.pallas_call(
        functools.partial(kernel, n_dp, n_chan, patches, width, scale),
        out_shape=(
            jax.ShapeDtypeStruct((patches, images, local), BF16),
            jax.ShapeDtypeStruct((2 * rows, 256), F32),
            jax.ShapeDtypeStruct((2 * rows, patches), F32),
            jax.ShapeDtypeStruct((2, local), F32),
        ),
        in_specs=[hbm, hbm] + [vmem] * 5,
        out_specs=(vmem, vmem, vmem, vmem),
        scratch_shapes=[
            pltpu.VMEM((patches, images, local), BF16),
            pltpu.VMEM((patches, images, local), BF16),
            pltpu.VMEM((PP, images * local), BF16),
            pltpu.VMEM((PP, images * local), BF16),
            pltpu.VMEM((hid, images * local), F32),
            pltpu.VMEM((hid, images * local), BF16),
            pltpu.VMEM((hid // 2, NB * local), BF16),
            pltpu.VMEM((chunks, patches * NB, local), F32),
            pltpu.VMEM((chunks, patches * NB, local), F32),
            pltpu.VMEM((16 * NB, local), F32),
            pltpu.VMEM((chunks, NB, 2 * LANES), F32),
            pltpu.VMEM((2, groups, 2, rows, 4 * LANES), F32),
            pltpu.VMEM(stat, F32),
            pltpu.VMEM((chunks, n_chan, NB, 4 * LANES), F32),
            pltpu.VMEM(stat, F32),
            pltpu.VMEM((chunks, n_chan, NB, 4 * LANES), F32),
            pltpu.VMEM((2, groups, rows, 4 * LANES), F32),
            pltpu.VMEM((2, groups, rows, 4 * LANES), F32),
            pltpu.VMEM((2, groups, rows, 4 * LANES), F32),
            pltpu.VMEM((2, rows, 4 * LANES), F32),
            pltpu.VMEM((2, n_chan, rows, 4 * LANES), F32),
            pltpu.VMEM((2, local), F32),
            pltpu.VMEM((n_dp, 2, local), F32),
            dma((2, chunks)),
            dma((chunks, n_chan)),
            dma((chunks, n_chan)),
            dma((chunks, n_chan)),
            dma((chunks, n_chan)),
            dma((2,)),
            dma((2,)),
            dma((2, groups)),
            dma((2, groups)),
            dma((2, n_chan)),
            dma((2, n_chan)),
            dma((n_dp,)),
            dma((n_dp,)),
        ],
        compiler_params=pltpu.CompilerParams(
            collective_id=0, has_side_effects=True, vmem_limit_bytes=64_000_000
        ),
    )(
        inputs.transpose(1, 0, 2),
        upstream.transpose(1, 0, 2),
        norm_gain.reshape(1, local),
        norm_bias.reshape(1, local),
        w1a,
        w1t,
        w2t,
    )
    return (
        out.transpose(1, 0, 2),
        first[:, :patches],
        second.T,
        first[:, patches],
        vec[0],
        vec[1],
    )


def solution(mesh):
    in_specs = (P("dp", None, "chan"), P("chan"), P("chan"), P(), P(), P(), P("dp", None, "chan"))
    out_specs = (P("dp", None, "chan"), P("dp", None), P(None, "dp"), P("dp"), P("chan"), P("chan"))
    body = functools.partial(per_device, mesh.shape["dp"], mesh.shape["chan"])
    return jax.shard_map(
        body, mesh=mesh, in_specs=in_specs, out_specs=out_specs, check_vma=False
    )
```

```python
import functools

import jax
import jax.numpy as jnp
from jax import lax
from jax.experimental import pallas as pl
from jax.experimental.pallas import tpu as pltpu
from jax.sharding import PartitionSpec as P

EPS = 1e-06
NB = 16
PP = 208
LANES = 128
UG = 4
VMEM_LIMIT = 52_000_000
UH = 4
UB = 4
F32 = jnp.float32
BF16 = jnp.bfloat16


def contract_lanes(a, b):
    return lax.dot_general(a, b, (((1,), (1,)), ((), ())), preferred_element_type=F32)


def kernel(
    n_dp, n_chan, patches, width, scale,
    x_hbm, u_hbm, gain_ref, bias_ref, w1_ref, bf_ref, w2_ref,
    out_ref, first_ref, second_ref, first_b_ref, gain_g_ref, shift_g_ref,
    w1f, w2f, wtail, w1a, w1t, w2t,
    x_v, u_v, mx, up, ga, gp, act, normed_n, gm_n, tmp, inv_d, acc,
    a_send, a_recv, b_send, b_recv, p0_recv, csum, c1_recv, c1_sum, c2_recv, d_send, d_recv,
    load_sem, as_sem, ar_sem, bs_sem, br_sem, p0s_sem, p0r_sem, c1s_sem, c1r_sem, c2s_sem, c2r_sem, ds_sem, dr_sem,
):
    me_d = lax.axis_index("dp")
    me_c = lax.axis_index("chan")
    core = lax.rem(me_d, 2)
    me_g = lax.div(me_d, 2)
    groups = n_dp // 2
    chunks = x_v.shape[1] // NB
    hid = w1_ref.shape[1]
    half = hid // 2
    tiles = NB // 2
    span = NB * LANES

    def chan_peer(j):
        return lax.rem(me_c + j, n_chan)

    def dp_peer(j):
        return lax.rem(me_d + j, n_dp)

    def remote(src, dst, ssem, rsem, dp, chan):
        return pltpu.make_async_remote_copy(
            src_ref=src, dst_ref=dst, send_sem=ssem, recv_sem=rsem,
            device_id={"dp": dp, "chan": chan}, device_id_type=pl.DeviceIdType.MESH,
        )

    barrier = pltpu.get_barrier_semaphore()
    for j in range(1, n_chan):
        pl.semaphore_signal(barrier, inc=1, device_id={"dp": me_d, "chan": chan_peer(j)}, device_id_type=pl.DeviceIdType.MESH)
    for j in range(1, n_dp):
        pl.semaphore_signal(barrier, inc=1, device_id={"dp": dp_peer(j), "chan": me_c}, device_id_type=pl.DeviceIdType.MESH)

    def load(which, src, dst, part):
        lo = part * 64
        rows = pl.ds(lo, 64 if part < 2 else patches - lo)
        return pltpu.make_async_copy(src.at[rows], dst.at[rows], load_sem.at[which, part])

    for part in range(3):
        load(0, x_hbm, x_v, part).start()
    for part in range(3):
        load(1, u_hbm, u_v, part).start()

    lane = lax.broadcasted_iota(jnp.int32, (NB, LANES), 1)

    def lane_tiles(body, init):
        out = []
        for lo in range(0, patches, LANES):
            count = min(LANES, patches - lo)
            unroll = 32 if count == LANES else 34

            def step(q, carry, lo=lo, unroll=unroll):
                for i in range(unroll):
                    carry = body(lo + q * unroll + i, q * unroll + i, carry)
                return carry

            out.append(lax.fori_loop(0, count // unroll, step, init))
        return out

    zero = jnp.zeros((NB, LANES), F32)

    images = x_v.shape[1]
    wide = lax.broadcasted_iota(jnp.int32, (images, LANES), 1)
    stats = (jnp.zeros((images, LANES), F32),) * 2
    for part in range(3):
        load(0, x_hbm, x_v, part).wait()
        lo = part * 64
        unroll = 16 if part < 2 else 17
        count = (64 if part < 2 else patches - lo) // unroll

        def stat(q, carry, lo=lo, unroll=unroll):
            s, sq = carry
            for i in range(unroll):
                p = lo + q * unroll + i
                v = x_v[p].astype(F32)
                hit = wide == lax.rem(p, LANES)
                s = jnp.where(hit, jnp.sum(v, axis=-1, keepdims=True), s)
                sq = jnp.where(hit, jnp.sum(v * v, axis=-1, keepdims=True), sq)
            return s, sq

        stats = lax.fori_loop(0, count, stat, stats)
        if part:
            t = part - 1
            for ch in range(chunks):
                a_send[ch, :, pl.ds(t * LANES, LANES)] = stats[0][ch * NB : (ch + 1) * NB]
                a_send[ch, :, pl.ds((2 + t) * LANES, LANES)] = stats[1][ch * NB : (ch + 1) * NB]
    pl.semaphore_wait(barrier, n_chan - 1 + n_dp - 1)
    for ch in range(chunks):
        for j in range(1, n_chan):
            remote(a_send.at[ch], a_recv.at[ch, j], as_sem.at[ch, j], ar_sem.at[ch, j], me_d, chan_peer(j)).start()

    def select(lo, count):
        at = lo + lax.broadcasted_iota(jnp.int32, (count, hid), 0)
        h, rest_ = at // half, at % half
        unit = rest_ // 8 * 16 + h * 8 + rest_ % 8
        return jnp.where(lax.broadcasted_iota(jnp.int32, (count, hid), 1) == unit, 1.0, 0.0).astype(BF16)

    tail = patches // 16 * 16
    left = patches - tail
    for ref, dst in ((w1_ref, w1f), (w2_ref, w2f)):
        dst[pl.ds(0, tail), :] = ref[pl.ds(0, tail), :]
        wtail[...] = jnp.zeros((16, hid), F32)
        wtail[pl.ds(0, left), :] = ref[pl.ds(tail, left), :].astype(F32)
        if ref is w1_ref:
            rem = bf_ref[...]
            for i in range(3):
                piece = rem.astype(BF16).astype(F32)
                wtail[pl.ds(left + i, 1), :] = piece
                rem = rem - piece
        dst[pl.ds(tail, 16), :] = wtail[...].astype(BF16)
    for h in range(2):
        pick = select(h * half, half)
        rows = pl.ds(h * half, half)
        w1a[rows, :] = contract_lanes(pick, w1f[...]).astype(BF16)
        w2t[rows, :] = contract_lanes(pick, w2f[...]).astype(BF16)
        w1t[:, rows] = contract_lanes(w1f[pl.ds(0, patches), :], pick).astype(BF16)

    def regroup(g, ch, dst, value, fill):
        for i in range(16):
            tmp[pl.ds(i * NB, NB), :] = value(i)
        for b in range(NB):
            v = tmp[pl.ds(b, 16, stride=NB), :]
            if fill is not None:
                v = fill(v)
            at = pl.multiple_of(ch * span + b * LANES, LANES)
            rows = pl.ds(pl.multiple_of(g * 16, 16), 16)
            dst[rows, pl.ds(at, LANES)] = v.astype(BF16)

    full = patches // 16
    rest = patches - full * 16
    sub = lax.broadcasted_iota(jnp.int32, (16, LANES), 0)

    for part in range(3):
        load(1, u_hbm, u_v, part).wait()
    for ch in range(chunks):

        def up_group(g, _, ch=ch):
            regroup(g, ch, up, lambda i: u_v[g * 16 + i, pl.ds(ch * NB, NB), :].astype(F32), None)
            return 0

        lax.fori_loop(0, full, up_group, 0)
        regroup(
            full, ch, up,
            lambda i, ch=ch: u_v[full * 16 + min(i, rest - 1), pl.ds(ch * NB, NB), :].astype(F32),
            lambda v: jnp.where(sub < rest, v, 0.0),
        )

    def ga_tile(n, _):
        at = pl.ds(pl.multiple_of(n * 256, 256), 256)
        ga[:, at] = jnp.dot(w2t[...], up[:, at], preferred_element_type=F32)
        return 0

    lax.fori_loop(0, chunks * tiles, ga_tile, 0, unroll=UG)

    owned_b = []

    gain = gain_ref[...]
    bias = bias_ref[...]

    def wait_a(ch):
        total = a_send[ch]
        for j in range(1, n_chan):
            remote(a_send.at[ch], a_recv.at[ch, j], as_sem.at[ch, j], ar_sem.at[ch, j], me_d, chan_peer(j)).wait_recv()
            total = total + a_recv[ch, j]
        mean = total[:, : 2 * LANES] / width
        var = total[:, 2 * LANES :] / width - mean * mean
        return mean, lax.rsqrt(var + EPS)

    def column(value, i):
        return jnp.broadcast_to(value[:, i : i + 1], (NB, LANES))

    def normalise(ch):
        mean, inv = wait_a(ch)
        inv_d[ch] = inv
        mean_ref, inv_ref = a_send.at[ch], inv_d.at[ch]

        def one(g, mean16, inv16, count):
            def value(i):
                i = min(i, count - 1)
                p = g * 16 + i
                v = x_v[p, pl.ds(ch * NB, NB), :].astype(F32)
                normed = (v - column(mean16, i)) * column(inv16, i)
                normed_n[ch, pl.ds(pl.multiple_of(p * NB, NB), NB), :] = normed
                return normed * gain + bias

            fill = None
            if count < 16:
                fill = lambda v: jnp.where(sub < rest, v, jnp.where(sub < rest + 3, 1.0, 0.0))
            regroup(g, ch, mx, value, fill)

        for t in range(2):
            m_t = mean[:, t * LANES : (t + 1) * LANES]
            i_t = inv[:, t * LANES : (t + 1) * LANES]
            per = LANES // 16

            def group(g, carry, t=t):
                m, v = carry
                one(t * per + g, m, v, 16)
                return pltpu.roll(m, LANES - 16, 1), pltpu.roll(v, LANES - 16, 1)

            m_t, i_t = lax.fori_loop(0, min(per, full - t * per), group, (m_t, i_t))
        one(full, m_t, i_t, rest)

    def hidden(h, ch):
        rows = pl.ds(h * half, half)

        def tile(n, _):
            at = pl.ds(pl.multiple_of(ch * span + n * 256, 256), 256)
            pre = jnp.dot(w1a[rows, :], mx[:, at], preferred_element_type=F32)
            t = pre * 0.7071067811865476
            cdf = 0.5 * lax.erf(t) + 0.5
            act[:, pl.ds(pl.multiple_of(n * 256, 256), 256)] = (pre * cdf).astype(BF16)
            slope = cdf + (t * 0.5641895835477563) * jnp.exp(-(t * t))
            gp[rows, at] = (ga[rows, at] * slope).astype(BF16)
            return 0

        lax.fori_loop(0, tiles, tile, 0, unroll=UH)
        at = pl.ds(ch * span, span)
        first = contract_lanes(gp[rows, at], mx[:, at]).reshape(groups, 2, -1, PP)
        second = contract_lanes(act[...], up[:, at]).reshape(groups, 2, -1, PP)
        if ch:
            first = first + acc[h, :, :, :, pl.ds(0, PP)]
            second = second + acc[h, :, :, :, pl.ds(256, PP)]
        acc[h, :, :, :, pl.ds(0, PP)] = first
        acc[h, :, :, :, pl.ds(256, PP)] = second

    def p0(h):
        return remote(acc.at[h, :, 1 - core], p0_recv.at[h], p0s_sem.at[h], p0r_sem.at[h], me_d + 1 - 2 * core, me_c)

    def c1(h, j):
        g = lax.rem(me_g + j, groups)
        return remote(csum.at[h, g], c1_recv.at[h, me_g], c1s_sem.at[h, j], c1r_sem.at[h, me_g], 2 * g + core, me_c)

    def c1_arrival(h, j):
        g = lax.rem(me_g + j, groups)
        return remote(csum.at[h, g], c1_recv.at[h, g], c1s_sem.at[h, j], c1r_sem.at[h, g], 2 * g + core, me_c)

    def c2(h, j):
        return remote(c1_sum.at[h], c2_recv.at[h, me_c], c2s_sem.at[h, j], c2r_sem.at[h, me_c], me_d, chan_peer(j))

    def c2_arrival(h, j):
        c = chan_peer(j)
        return remote(c1_sum.at[h], c2_recv.at[h, c], c2s_sem.at[h, j], c2r_sem.at[h, c], me_d, c)

    def pair_done(h):
        p0(h).wait()
        csum[h] = acc[h, :, core] + p0_recv[h]
        for j in range(1, groups):
            c1(h, j).start()

    def group_done(h):
        c1_recv[h, me_g] = csum[h, me_g]
        for j in range(1, groups):
            c1_arrival(h, j).wait_recv()
        total = c1_recv[h, 0]
        for g in range(1, groups):
            total = total + c1_recv[h, g]
        c1_sum[h] = total
        c2_recv[h, me_c] = total
        for j in range(1, n_chan):
            c2(h, j).start()

    def all_done(h):
        for j in range(1, n_chan):
            c2_arrival(h, j).wait_recv()
        total = c2_recv[h, 0]
        for c in range(1, n_chan):
            total = total + c2_recv[h, c]
        total = total * scale
        first_ref[pl.ds(h * 8, 8), :] = total[:, :patches]
        here = lax.broadcasted_iota(jnp.int32, (8, LANES), 0) + h * 8 == lax.broadcasted_iota(jnp.int32, (8, LANES), 1)
        owned_b.append(jnp.sum(jnp.where(here, total[:, patches : patches + 1], 0.0), axis=0, keepdims=True))
        second_ref[pl.ds(h * 8, 8), :] = total[:, 256 : 256 + patches]

    for ch in range(chunks):
        normalise(ch)
    for ch in range(chunks):
        hidden(0, ch)
    p0(0).start()
    for ch in range(chunks):
        hidden(1, ch)
        if ch == 0:
            pair_done(0)
    p0(1).start()

    grads = (zero, zero)
    for ch in range(chunks):

        def back(n, _, ch=ch):
            at = pl.ds(pl.multiple_of(ch * span + n * 256, 256), 256)
            gm = jnp.dot(w1t[...], gp[:, at], preferred_element_type=F32)
            for i in range(2):
                gm_n[ch, pl.ds(n * 2 + i, patches, stride=NB), :] = gm[:, i * LANES : (i + 1) * LANES]
            return 0

        lax.fori_loop(0, tiles, back, 0, unroll=UB)

        def sums(p, at, carry, ch=ch):
            f, s, dg, ds = carry
            rows = pl.ds(pl.multiple_of(p * NB, NB), NB)
            gm = gm_n[ch, rows, :]
            normed = normed_n[ch, rows, :]
            both = gm * normed
            hit = lane == at
            f = jnp.where(hit, jnp.sum(gm * gain, axis=-1, keepdims=True), f)
            s = jnp.where(hit, jnp.sum(both * gain, axis=-1, keepdims=True), s)
            return f, s, dg + both, ds + gm

        for t, (f, s, dg, ds) in enumerate(lane_tiles(sums, (zero, zero, zero, zero))):
            b_send[ch, :, pl.ds(t * LANES, LANES)] = f
            b_send[ch, :, pl.ds((2 + t) * LANES, LANES)] = s
            grads = (grads[0] + dg, grads[1] + ds)
        for j in range(1, n_chan):
            remote(b_send.at[ch], b_recv.at[ch, j], bs_sem.at[ch, j], br_sem.at[ch, j], me_d, chan_peer(j)).start()
        if ch == 0:
            pair_done(1)

    mine = jnp.concatenate([jnp.sum(v, axis=0, keepdims=True) for v in grads], axis=0)
    d_send[...] = mine
    d_recv[me_d] = mine
    for j in range(1, n_dp):
        remote(d_send, d_recv.at[me_d], ds_sem.at[j], dr_sem.at[me_d], dp_peer(j), me_c).start()
    group_done(0)

    for ch in range(chunks):
        total = b_send[ch]
        for j in range(1, n_chan):
            remote(b_send.at[ch], b_recv.at[ch, j], bs_sem.at[ch, j], br_sem.at[ch, j], me_d, chan_peer(j)).wait_recv()
            total = total + b_recv[ch, j]
        inv = inv_d[ch]
        f = total[:, : 2 * LANES] * inv / width
        s = total[:, 2 * LANES :] * inv / width

        for t in range(2):
            lo = t * LANES
            count = min(LANES, patches - lo)
            cut = slice(lo, lo + LANES)

            unroll = 32 if count == LANES else 34

            def finish(q, carry, ch=ch, lo=lo, unroll=unroll):
                i_t, f_t, s_t = carry
                for i in range(unroll):
                    p = lo + q * unroll + i
                    rows = pl.ds(pl.multiple_of(p * NB, NB), NB)
                    bs = pl.ds(ch * NB, NB)
                    gn = gm_n[ch, rows, :] * gain
                    v = u_v[p, bs, :].astype(F32) + column(i_t, i) * gn - column(f_t, i) - column(s_t, i) * normed_n[ch, rows, :]
                    out_ref[p, bs, :] = v.astype(BF16)
                return tuple(pltpu.roll(c, LANES - unroll, 1) for c in carry)

            lax.fori_loop(0, count // unroll, finish, (inv[:, cut], f[:, cut], s[:, cut]))

    group_done(1)
    all_done(0)
    for j in range(1, n_dp):
        d = dp_peer(j)
        remote(d_send, d_recv.at[d], ds_sem.at[j], dr_sem.at[d], d, me_c).wait_recv()
    vec = d_recv[0]
    for d in range(1, n_dp):
        vec = vec + d_recv[d]
    gain_g_ref[...] = vec[0:1] * scale
    shift_g_ref[...] = vec[1:2] * scale
    all_done(1)
    first_b_ref[...] = (owned_b[0] + owned_b[1])[:, :16]

    for ch in range(chunks):
        for j in range(1, n_chan):
            remote(a_send.at[ch], a_recv.at[ch, j], as_sem.at[ch, j], ar_sem.at[ch, j], me_d, chan_peer(j)).wait_send()
            remote(b_send.at[ch], b_recv.at[ch, j], bs_sem.at[ch, j], br_sem.at[ch, j], me_d, chan_peer(j)).wait_send()
    for h in range(2):
        for j in range(1, groups):
            c1(h, j).wait_send()
        for j in range(1, n_chan):
            c2(h, j).wait_send()
    for j in range(1, n_dp):
        remote(d_send, d_recv.at[me_d], ds_sem.at[j], dr_sem.at[me_d], dp_peer(j), me_c).wait_send()


def per_device(n_dp, n_chan, inputs, norm_gain, norm_bias, w_first, b_first, w_second, upstream):
    images, patches, local = inputs.shape
    hid = w_first.shape[0]
    groups = n_dp // 2
    chunks = images // NB
    width = float(local * n_chan)
    scale = 1.0 / (images * n_dp)
    rows = hid // (groups * 4)
    stat = (chunks, NB, 4 * LANES)
    vmem = pl.BlockSpec(memory_space=pltpu.VMEM)
    hbm = pl.BlockSpec(memory_space=pltpu.HBM)
    dma = pltpu.SemaphoreType.DMA
    out, first, second, first_b, gain_g, shift_g = pl.pallas_call(
        functools.partial(kernel, n_dp, n_chan, patches, width, scale),
        out_shape=(
            jax.ShapeDtypeStruct((patches, images, local), BF16),
            jax.ShapeDtypeStruct((2 * rows, patches), F32),
            jax.ShapeDtypeStruct((2 * rows, patches), F32),
            jax.ShapeDtypeStruct((1, 2 * rows), F32),
            jax.ShapeDtypeStruct((1, local), F32),
            jax.ShapeDtypeStruct((1, local), F32),
        ),
        in_specs=[hbm, hbm] + [vmem] * 5,
        out_specs=(vmem,) * 6,
        scratch_shapes=[
            pltpu.VMEM((PP, hid), BF16),
            pltpu.VMEM((PP, hid), BF16),
            pltpu.VMEM((16, hid), F32),
            pltpu.VMEM((hid, PP), BF16),
            pltpu.VMEM((patches, hid), BF16),
            pltpu.VMEM((hid, PP), BF16),
            pltpu.VMEM((patches, images, local), BF16),
            pltpu.VMEM((patches, images, local), BF16),
            pltpu.VMEM((PP, images * local), BF16),
            pltpu.VMEM((PP, images * local), BF16),
            pltpu.VMEM((hid, images * local), F32),
            pltpu.VMEM((hid, images * local), BF16),
            pltpu.VMEM((hid // 2, NB * local), BF16),
            pltpu.VMEM((chunks, patches * NB, local), F32),
            pltpu.VMEM((chunks, patches * NB, local), F32),
            pltpu.VMEM((16 * NB, local), F32),
            pltpu.VMEM((chunks, NB, 2 * LANES), F32),
            pltpu.VMEM((2, groups, 2, rows, 4 * LANES), F32),
            pltpu.VMEM(stat, F32),
            pltpu.VMEM((chunks, n_chan, NB, 4 * LANES), F32),
            pltpu.VMEM(stat, F32),
            pltpu.VMEM((chunks, n_chan, NB, 4 * LANES), F32),
            pltpu.VMEM((2, groups, rows, 4 * LANES), F32),
            pltpu.VMEM((2, groups, rows, 4 * LANES), F32),
            pltpu.VMEM((2, groups, rows, 4 * LANES), F32),
            pltpu.VMEM((2, rows, 4 * LANES), F32),
            pltpu.VMEM((2, n_chan, rows, 4 * LANES), F32),
            pltpu.VMEM((2, local), F32),
            pltpu.VMEM((n_dp, 2, local), F32),
            dma((2, 3)),
            dma((chunks, n_chan)),
            dma((chunks, n_chan)),
            dma((chunks, n_chan)),
            dma((chunks, n_chan)),
            dma((2,)),
            dma((2,)),
            dma((2, groups)),
            dma((2, groups)),
            dma((2, n_chan)),
            dma((2, n_chan)),
            dma((n_dp,)),
            dma((n_dp,)),
        ],
        compiler_params=pltpu.CompilerParams(
            collective_id=0, has_side_effects=True, vmem_limit_bytes=VMEM_LIMIT
        ),
    )(
        inputs.transpose(1, 0, 2),
        upstream.transpose(1, 0, 2),
        norm_gain.reshape(1, local),
        norm_bias.reshape(1, local),
        w_first.T,
        b_first.reshape(1, hid),
        w_second,
    )
    return (
        out.transpose(1, 0, 2),
        first,
        second.T,
        first_b[0],
        gain_g[0],
        shift_g[0],
    )


def solution(mesh):
    in_specs = (P("dp", None, "chan"), P("chan"), P("chan"), P(), P(), P(), P("dp", None, "chan"))
    out_specs = (P("dp", None, "chan"), P("dp", None), P(None, "dp"), P("dp"), P("chan"), P("chan"))
    body = functools.partial(per_device, mesh.shape["dp"], mesh.shape["chan"])
    return jax.shard_map(
        body, mesh=mesh, in_specs=in_specs, out_specs=out_specs, check_vma=False
    )
```

```python
import functools

import jax
import jax.numpy as jnp
from jax import lax
from jax.experimental import pallas as pl
from jax.experimental.pallas import tpu as pltpu
from jax.sharding import PartitionSpec as P

EPS = 1e-06
NB = 16
PP = 208
LANES = 128
UG = 8
US = 4
UN = 6
UR = 8
UF = 8
VMEM_LIMIT = 51_500_000
UH = 8
F32 = jnp.float32
BF16 = jnp.bfloat16


def contract_lanes(a, b):
    return lax.dot_general(a, b, (((1,), (1,)), ((), ())), preferred_element_type=F32)


def kernel(
    n_dp, n_chan, patches, width, scale,
    x_hbm, u_hbm, gain_hbm, bias_hbm, w1_hbm, bf_hbm, w2_hbm,
    out_ref, first_ref, second_ref, first_b_ref, gain_g_ref, shift_g_ref,
    gain_ref, bias_ref, w1_ref, bf_ref, w2_ref, w1f, w2f, wtail, w1a, w1t, w2t,
    x_v, u_v, mx, up, ga, gp, act, normed_n, inv_n, gm_n, tmp, mean_d, inv_d, first_d, second_d, acc,
    a_send, a_recv, b_send, b_recv, p0_recv, csum, c1_recv, c1_sum, c2_recv, d_send, d_recv,
    load_sem, small_sem, as_sem, ar_sem, bs_sem, br_sem, p0s_sem, p0r_sem, c1s_sem, c1r_sem, c2s_sem, c2r_sem, ds_sem, dr_sem,
):
    me_d = lax.axis_index("dp")
    me_c = lax.axis_index("chan")
    core = lax.rem(me_d, 2)
    me_g = lax.div(me_d, 2)
    groups = n_dp // 2
    chunks = x_v.shape[1] // NB
    hid = w1_hbm.shape[1]
    half = hid // 2
    tiles = NB // 2
    span = NB * LANES

    def chan_peer(j):
        return lax.rem(me_c + j, n_chan)

    def dp_peer(j):
        return lax.rem(me_d + j, n_dp)

    def remote(src, dst, ssem, rsem, dp, chan):
        return pltpu.make_async_remote_copy(
            src_ref=src, dst_ref=dst, send_sem=ssem, recv_sem=rsem,
            device_id={"dp": dp, "chan": chan}, device_id_type=pl.DeviceIdType.MESH,
        )

    barrier = pltpu.get_barrier_semaphore()
    for j in range(1, n_chan):
        pl.semaphore_signal(barrier, inc=1, device_id={"dp": me_d, "chan": chan_peer(j)}, device_id_type=pl.DeviceIdType.MESH)
    for j in range(1, n_dp):
        pl.semaphore_signal(barrier, inc=1, device_id={"dp": dp_peer(j), "chan": me_c}, device_id_type=pl.DeviceIdType.MESH)

    def load(which, src, dst, part):
        lo = part * 64
        rows = pl.ds(lo, 64 if part < 2 else patches - lo)
        return pltpu.make_async_copy(src.at[rows], dst.at[rows], load_sem.at[which, part])

    for part in range(3):
        load(0, x_hbm, x_v, part).start()
    small = [
        pltpu.make_async_copy(src, dst, small_sem.at[i])
        for i, (src, dst) in enumerate(
            ((w1_hbm, w1_ref), (w2_hbm, w2_ref), (bf_hbm, bf_ref), (gain_hbm, gain_ref), (bias_hbm, bias_ref))
        )
    ]
    for copy in small:
        copy.start()
    for part in range(3):
        load(1, u_hbm, u_v, part).start()

    blocks = -(-patches // 8)
    second_row = -(-blocks // 8) * 8
    eye = lax.broadcasted_iota(jnp.int32, (LANES, LANES), 0) == lax.broadcasted_iota(jnp.int32, (LANES, LANES), 1)

    def dense(value):
        n = value.shape[0]
        return jnp.sum(jnp.where(eye[:n], value, 0.0), axis=0, keepdims=True)

    def spread(row):
        return jnp.broadcast_to(row, (LANES, LANES)).T

    def over_blocks(body, init, lo=0, hi=None, unroll=4):
        hi = blocks if hi is None else hi
        whole = min(hi, patches // 8) - lo

        def step(i, carry):
            for k in range(unroll):
                carry = body(lo + i * unroll + k, LANES, carry)
            return carry

        carry = lax.fori_loop(0, whole // unroll, step, init)
        for k in range(whole // unroll * unroll, whole):
            carry = body(lo + k, LANES, carry)
        if hi > patches // 8:
            carry = body(hi - 1, (patches % 8) * NB, carry)
        return carry

    def images_of(ref, g, n, ch):
        return ref[pl.ds(g * 8, n // NB), pl.ds(ch * NB, NB), :].reshape(n, LANES)

    ones = jnp.ones((LANES, LANES), BF16)
    for part in range(3):
        load(0, x_hbm, x_v, part).wait()

        def stat(g, n, carry):
            for ch in range(chunks):
                v = images_of(x_v, g, n, ch)
                total = jnp.dot(v, ones, preferred_element_type=F32)
                v = v.astype(F32)
                a_send[ch, pl.ds(g, 1), :] = dense(total)
                squares = jnp.broadcast_to(jnp.sum(v * v, axis=-1, keepdims=True), (n, LANES))
                a_send[ch, pl.ds(second_row + g, 1), :] = dense(squares)
            return carry

        over_blocks(stat, 0, part * 8, part * 8 + 8 if part < 2 else None, US)
    pl.semaphore_wait(barrier, n_chan - 1 + n_dp - 1)
    for ch in range(chunks):
        for j in range(1, n_chan):
            remote(a_send.at[ch], a_recv.at[ch, j], as_sem.at[ch, j], ar_sem.at[ch, j], me_d, chan_peer(j)).start()

    def select(lo, count):
        at = lo + lax.broadcasted_iota(jnp.int32, (count, hid), 0)
        h, rest_ = at // half, at % half
        unit = rest_ // 8 * 16 + h * 8 + rest_ % 8
        return jnp.where(lax.broadcasted_iota(jnp.int32, (count, hid), 1) == unit, 1.0, 0.0).astype(BF16)

    for copy in small:
        copy.wait()
    tail = patches // 16 * 16
    left = patches - tail
    for ref, dst in ((w1_ref, w1f), (w2_ref, w2f)):
        dst[pl.ds(0, tail), :] = ref[pl.ds(0, tail), :]
        wtail[...] = jnp.zeros((16, hid), F32)
        wtail[pl.ds(0, left), :] = ref[pl.ds(tail, left), :].astype(F32)
        if ref is w1_ref:
            rem = bf_ref[...]
            for i in range(3):
                piece = rem.astype(BF16).astype(F32)
                wtail[pl.ds(left + i, 1), :] = piece
                rem = rem - piece
        dst[pl.ds(tail, 16), :] = wtail[...].astype(BF16)
    for h in range(2):
        pick = select(h * half, half)
        rows = pl.ds(h * half, half)
        w1a[rows, :] = contract_lanes(pick, w1f[...]).astype(BF16)
        w2t[rows, :] = contract_lanes(pick, w2f[...]).astype(BF16)
        w1t[:, rows] = contract_lanes(w1f[pl.ds(0, patches), :], pick).astype(BF16)

    tmp[...] = jnp.zeros_like(tmp)
    def ungroup(g, ch, dst, fill):
        for b in range(NB):
            v = tmp[pl.ds(b, 16, stride=NB), :]
            if fill is not None:
                v = fill(v)
            at = pl.multiple_of(ch * span + b * LANES, LANES)
            rows = pl.ds(pl.multiple_of(g * 16, 16), 16)
            dst[rows, pl.ds(at, LANES)] = v.astype(BF16)

    full = patches // 16
    rest = patches - full * 16
    sub = lax.broadcasted_iota(jnp.int32, (16, LANES), 0)

    for part in range(3):
        load(1, u_hbm, u_v, part).wait()
    for ch in range(chunks):

        def up_group(g, _, ch=ch):
            tmp[...] = u_v[pl.ds(g * 16, 16), pl.ds(ch * NB, NB), :].reshape(16 * NB, LANES).astype(F32)
            ungroup(g, ch, up, None)
            return 0

        lax.fori_loop(0, full, up_group, 0)
        tmp[pl.ds(0, rest * NB), :] = images_of(u_v, full * 2, rest * NB, ch).astype(F32)
        ungroup(full, ch, up, lambda v: jnp.where(sub < rest, v, 0.0))

    def ga_tile(n, _):
        at = pl.ds(pl.multiple_of(n * 256, 256), 256)
        ga[:, at] = jnp.dot(w2t[...], up[:, at], preferred_element_type=F32).astype(BF16)
        return 0

    lax.fori_loop(0, chunks * tiles, ga_tile, 0, unroll=UG)

    owned_b = []

    gain = gain_ref[...]
    bias = bias_ref[...]

    def received(send, recv, ssem, rsem, ch):
        for j in range(1, n_chan):
            remote(send.at[ch], recv.at[ch, j], ssem.at[ch, j], rsem.at[ch, j], me_d, chan_peer(j)).wait_recv()
        totals = []
        for lo in (0, second_row):
            total = send[ch, pl.ds(lo, blocks), :]
            for j in range(1, n_chan):
                total = total + recv[ch, j, pl.ds(lo, blocks), :]
            totals.append(total)
        return totals

    def normalise(ch):
        total, squares = received(a_send, a_recv, as_sem, ar_sem, ch)
        mean = total / width
        mean_d[ch] = mean
        inv_d[ch] = lax.rsqrt(squares / width - mean * mean + EPS)

        def block(g, n):
            m = spread(mean_d[ch, pl.ds(g, 1), :])[:n]
            inv = spread(inv_d[ch, pl.ds(g, 1), :])[:n]
            rows = pl.ds(pl.multiple_of(g * LANES, 64), n)
            normed = (images_of(x_v, g, n, ch).astype(F32) - m) * inv
            normed_n[ch, rows, :] = normed
            inv_n[ch, rows, :] = inv
            return normed * gain + bias

        def pair(g, carry):
            for k in range(2):
                tmp[pl.ds(k * LANES, LANES), :] = block(g * 2 + k, LANES)
            ungroup(g, ch, mx, None)
            return carry

        lax.fori_loop(0, full, pair, 0, unroll=UN)
        tmp[pl.ds(0, rest * NB), :] = block(blocks - 1, rest * NB)
        ungroup(full, ch, mx, lambda v: jnp.where(sub < rest, v, jnp.where(sub < rest + 3, 1.0, 0.0)))

    def hidden(h, ch):
        rows = pl.ds(h * half, half)

        def tile(n, _):
            at = pl.ds(pl.multiple_of(ch * span + n * 256, 256), 256)
            pre = jnp.dot(w1a[rows, :], mx[:, at], preferred_element_type=F32)
            t = pre * 0.7071067811865476
            cdf = 0.5 * lax.erf(t) + 0.5
            act[:, pl.ds(pl.multiple_of(n * 256, 256), 256)] = (pre * cdf).astype(BF16)
            slope = cdf + (t * 0.5641895835477563) * jnp.exp(-(t * t))
            gp[rows, at] = (ga[rows, at].astype(F32) * slope).astype(BF16)
            return 0

        lax.fori_loop(0, tiles, tile, 0, unroll=UH)
        at = pl.ds(ch * span, span)
        first = contract_lanes(gp[rows, at], mx[:, at]).reshape(groups, 2, -1, PP)
        second = contract_lanes(act[...], up[:, at]).reshape(groups, 2, -1, PP)
        if ch:
            first = first + acc[h, :, :, :, pl.ds(0, PP)]
            second = second + acc[h, :, :, :, pl.ds(256, PP)]
        acc[h, :, :, :, pl.ds(0, PP)] = first
        acc[h, :, :, :, pl.ds(256, PP)] = second

    def p0(h):
        return remote(acc.at[h, :, 1 - core], p0_recv.at[h], p0s_sem.at[h], p0r_sem.at[h], me_d + 1 - 2 * core, me_c)

    def c1(h, j):
        g = lax.rem(me_g + j, groups)
        return remote(csum.at[h, g], c1_recv.at[h, me_g], c1s_sem.at[h, j], c1r_sem.at[h, me_g], 2 * g + core, me_c)

    def c1_arrival(h, j):
        g = lax.rem(me_g + j, groups)
        return remote(csum.at[h, g], c1_recv.at[h, g], c1s_sem.at[h, j], c1r_sem.at[h, g], 2 * g + core, me_c)

    def c2(h, j):
        return remote(c1_sum.at[h], c2_recv.at[h, me_c], c2s_sem.at[h, j], c2r_sem.at[h, me_c], me_d, chan_peer(j))

    def c2_arrival(h, j):
        c = chan_peer(j)
        return remote(c1_sum.at[h], c2_recv.at[h, c], c2s_sem.at[h, j], c2r_sem.at[h, c], me_d, c)

    def pair_done(h):
        p0(h).wait()
        csum[h] = acc[h, :, core] + p0_recv[h]
        for j in range(1, groups):
            c1(h, j).start()

    def group_done(h):
        c1_recv[h, me_g] = csum[h, me_g]
        for j in range(1, groups):
            c1_arrival(h, j).wait_recv()
        total = c1_recv[h, 0]
        for g in range(1, groups):
            total = total + c1_recv[h, g]
        c1_sum[h] = total
        c2_recv[h, me_c] = total
        for j in range(1, n_chan):
            c2(h, j).start()

    def all_done(h):
        for j in range(1, n_chan):
            c2_arrival(h, j).wait_recv()
        total = c2_recv[h, 0]
        for c in range(1, n_chan):
            total = total + c2_recv[h, c]
        total = total * scale
        first_ref[pl.ds(h * 8, 8), :] = total[:, :patches]
        here = lax.broadcasted_iota(jnp.int32, (8, LANES), 0) + h * 8 == lax.broadcasted_iota(jnp.int32, (8, LANES), 1)
        owned_b.append(jnp.sum(jnp.where(here, total[:, patches : patches + 1], 0.0), axis=0, keepdims=True))
        second_ref[pl.ds(h * 8, 8), :] = total[:, 256 : 256 + patches]

    for ch in range(chunks):
        normalise(ch)
    for ch in range(chunks):
        hidden(0, ch)
    p0(0).start()
    for ch in range(chunks):
        hidden(1, ch)
        if ch == 0:
            pair_done(0)
    p0(1).start()

    wide = lax.broadcasted_iota(jnp.int32, (16, 256), 0) == lax.broadcasted_iota(jnp.int32, (16, 256), 1) // LANES
    both_ones = jnp.where(wide, 1.0, 0.0).astype(BF16)

    def back(ch):
        for n in range(tiles):
            at = pl.ds(pl.multiple_of(ch * span + n * 256, 256), 256)
            gm = jnp.dot(w1t[...], gp[:, at], preferred_element_type=F32)
            for i in range(2):
                gm_n[ch, pl.ds(n * 2 + i, patches, stride=NB), :] = gm[:, i * LANES : (i + 1) * LANES]

    def row_sums(ch, grads):
        def sums(g, n, carry):
            dg, ds = carry
            rows = pl.ds(pl.multiple_of(g * LANES, 64), n)
            gm = gm_n[ch, rows, :]
            normed = normed_n[ch, rows, :]
            both = gm * normed
            gn = gm * gain
            gm_n[ch, rows, :] = gn * inv_n[ch, rows, :]
            pair = jnp.concatenate([gn.astype(BF16), (both * gain).astype(BF16)], axis=1)
            total = contract_lanes(both_ones, pair)
            b_send[ch, pl.ds(g, 1), :n] = total[0:1]
            b_send[ch, pl.ds(second_row + g, 1), :n] = total[1:2]
            return dg + both.reshape(-1, 8, LANES).sum(axis=0), ds + gm.reshape(-1, 8, LANES).sum(axis=0)

        grads = over_blocks(sums, grads, unroll=UR)
        for j in range(1, n_chan):
            remote(b_send.at[ch], b_recv.at[ch, j], bs_sem.at[ch, j], br_sem.at[ch, j], me_d, chan_peer(j)).start()
        return grads

    grads = (jnp.zeros((8, LANES), F32),) * 2
    back(0)
    pair_done(1)
    for ch in range(chunks):
        if ch:
            back(ch)
        grads = row_sums(ch, grads)

    mine = jnp.concatenate([jnp.sum(v, axis=0, keepdims=True) for v in grads], axis=0)
    d_send[...] = mine
    d_recv[me_d] = mine
    for j in range(1, n_dp):
        remote(d_send, d_recv.at[me_d], ds_sem.at[j], dr_sem.at[me_d], dp_peer(j), me_c).start()
    group_done(0)

    for ch in range(chunks):
        if ch == chunks - 1:
            group_done(1)
        totals = received(b_send, b_recv, bs_sem, br_sem, ch)
        for dst, total in zip((first_d, second_d), totals):
            dst[...] = total * inv_d[ch] / width

        def finish(g, n, carry, ch=ch):
            rows = pl.ds(pl.multiple_of(g * LANES, 64), n)
            f = spread(first_d[pl.ds(g, 1), :])[:n]
            q = spread(second_d[pl.ds(g, 1), :])[:n]
            v = images_of(u_v, g, n, ch).astype(F32) + gm_n[ch, rows, :] - f - q * normed_n[ch, rows, :]
            out_ref[pl.ds(g * 8, n // NB), pl.ds(ch * NB, NB), :] = v.astype(BF16).reshape(n // NB, NB, LANES)
            return carry

        over_blocks(finish, 0, unroll=UF)

    all_done(0)
    for j in range(1, n_dp):
        d = dp_peer(j)
        remote(d_send, d_recv.at[d], ds_sem.at[j], dr_sem.at[d], d, me_c).wait_recv()
    vec = d_recv[0]
    for d in range(1, n_dp):
        vec = vec + d_recv[d]
    gain_g_ref[...] = vec[0:1] * scale
    shift_g_ref[...] = vec[1:2] * scale
    all_done(1)
    first_b_ref[...] = (owned_b[0] + owned_b[1])[:, :16]

    for ch in range(chunks):
        for j in range(1, n_chan):
            remote(a_send.at[ch], a_recv.at[ch, j], as_sem.at[ch, j], ar_sem.at[ch, j], me_d, chan_peer(j)).wait_send()
            remote(b_send.at[ch], b_recv.at[ch, j], bs_sem.at[ch, j], br_sem.at[ch, j], me_d, chan_peer(j)).wait_send()
    for h in range(2):
        for j in range(1, groups):
            c1(h, j).wait_send()
        for j in range(1, n_chan):
            c2(h, j).wait_send()
    for j in range(1, n_dp):
        remote(d_send, d_recv.at[me_d], ds_sem.at[j], dr_sem.at[me_d], dp_peer(j), me_c).wait_send()


def per_device(n_dp, n_chan, inputs, norm_gain, norm_bias, w_first, b_first, w_second, upstream):
    images, patches, local = inputs.shape
    hid = w_first.shape[0]
    groups = n_dp // 2
    chunks = images // NB
    width = float(local * n_chan)
    scale = 1.0 / (images * n_dp)
    rows = hid // (groups * 4)
    blocks = -(-patches // 8)
    stat_rows = -(-blocks // 8) * 8 + blocks
    stat = (chunks, stat_rows, LANES)
    vmem = pl.BlockSpec(memory_space=pltpu.VMEM)
    hbm = pl.BlockSpec(memory_space=pltpu.HBM)
    dma = pltpu.SemaphoreType.DMA
    out, first, second, first_b, gain_g, shift_g = pl.pallas_call(
        functools.partial(kernel, n_dp, n_chan, patches, width, scale),
        out_shape=(
            jax.ShapeDtypeStruct((patches, images, local), BF16),
            jax.ShapeDtypeStruct((2 * rows, patches), F32),
            jax.ShapeDtypeStruct((2 * rows, patches), F32),
            jax.ShapeDtypeStruct((1, 2 * rows), F32),
            jax.ShapeDtypeStruct((1, local), F32),
            jax.ShapeDtypeStruct((1, local), F32),
        ),
        in_specs=[hbm] * 7,
        out_specs=(vmem,) * 6,
        scratch_shapes=[
            pltpu.VMEM((1, local), F32),
            pltpu.VMEM((1, local), F32),
            pltpu.VMEM((patches, hid), BF16),
            pltpu.VMEM((1, hid), F32),
            pltpu.VMEM((patches, hid), BF16),
            pltpu.VMEM((PP, hid), BF16),
            pltpu.VMEM((PP, hid), BF16),
            pltpu.VMEM((16, hid), F32),
            pltpu.VMEM((hid, PP), BF16),
            pltpu.VMEM((patches, hid), BF16),
            pltpu.VMEM((hid, PP), BF16),
            pltpu.VMEM((patches, images, local), BF16),
            pltpu.VMEM((patches, images, local), BF16),
            pltpu.VMEM((PP, images * local), BF16),
            pltpu.VMEM((PP, images * local), BF16),
            pltpu.VMEM((hid, images * local), BF16),
            pltpu.VMEM((hid, images * local), BF16),
            pltpu.VMEM((hid // 2, NB * local), BF16),
            pltpu.VMEM((chunks, patches * NB, local), F32),
            pltpu.VMEM((chunks, patches * NB, local), F32),
            pltpu.VMEM((chunks, patches * NB, local), F32),
            pltpu.VMEM((16 * NB, local), F32),
            pltpu.VMEM((chunks, blocks, LANES), F32),
            pltpu.VMEM((chunks, blocks, LANES), F32),
            pltpu.VMEM((blocks, LANES), F32),
            pltpu.VMEM((blocks, LANES), F32),
            pltpu.VMEM((2, groups, 2, rows, 4 * LANES), F32),
            pltpu.VMEM(stat, F32),
            pltpu.VMEM((chunks, n_chan, stat_rows, LANES), F32),
            pltpu.VMEM(stat, F32),
            pltpu.VMEM((chunks, n_chan, stat_rows, LANES), F32),
            pltpu.VMEM((2, groups, rows, 4 * LANES), F32),
            pltpu.VMEM((2, groups, rows, 4 * LANES), F32),
            pltpu.VMEM((2, groups, rows, 4 * LANES), F32),
            pltpu.VMEM((2, rows, 4 * LANES), F32),
            pltpu.VMEM((2, n_chan, rows, 4 * LANES), F32),
            pltpu.VMEM((2, local), F32),
            pltpu.VMEM((n_dp, 2, local), F32),
            dma((2, 3)),
            dma((5,)),
            dma((chunks, n_chan)),
            dma((chunks, n_chan)),
            dma((chunks, n_chan)),
            dma((chunks, n_chan)),
            dma((2,)),
            dma((2,)),
            dma((2, groups)),
            dma((2, groups)),
            dma((2, n_chan)),
            dma((2, n_chan)),
            dma((n_dp,)),
            dma((n_dp,)),
        ],
        compiler_params=pltpu.CompilerParams(
            collective_id=0, has_side_effects=True, vmem_limit_bytes=VMEM_LIMIT
        ),
    )(
        inputs.transpose(1, 0, 2),
        upstream.transpose(1, 0, 2),
        norm_gain.reshape(1, local),
        norm_bias.reshape(1, local),
        w_first.T,
        b_first.reshape(1, hid),
        w_second,
    )
    return (
        out.transpose(1, 0, 2),
        first,
        second.T,
        first_b[0],
        gain_g[0],
        shift_g[0],
    )


def solution(mesh):
    in_specs = (P("dp", None, "chan"), P("chan"), P("chan"), P(), P(), P(), P("dp", None, "chan"))
    out_specs = (P("dp", None, "chan"), P("dp", None), P(None, "dp"), P("dp"), P("chan"), P("chan"))
    body = functools.partial(per_device, mesh.shape["dp"], mesh.shape["chan"])
    return jax.shard_map(
        body, mesh=mesh, in_specs=in_specs, out_specs=out_specs, check_vma=False
    )
```

```python
import functools

import jax
import jax.numpy as jnp
from jax import lax
from jax.experimental import pallas as pl
from jax.experimental.pallas import tpu as pltpu
from jax.sharding import PartitionSpec as P

EPS = 1e-06
NB = 16
PP = 208
LANES = 128
UG = 8
US = 4
UN = 6
UR = 8
UF = 8
VMEM_LIMIT = 51_500_000
UH = 8
F32 = jnp.float32
BF16 = jnp.bfloat16


def contract_lanes(a, b):
    return lax.dot_general(a, b, (((1,), (1,)), ((), ())), preferred_element_type=F32)


def kernel(
    n_dp, n_chan, patches, width, scale,
    x_hbm, u_hbm, gain_hbm, bias_hbm, w1_hbm, bf_hbm, w2_hbm,
    out_ref, first_ref, second_ref, first_b_ref, gain_g_ref, shift_g_ref,
    gain_ref, bias_ref, w1_ref, bf_ref, w2_ref, w1f, w2f, wtail, w1a, w1t, w2t,
    x_v, u_v, mx, up, ga, gp, act, normed_n, inv_n, gm_n, tmp, mean_d, inv_d, first_d, second_d, acc,
    a_send, a_recv, b_send, b_recv, p0_recv, csum, c1_recv, c1_sum, c2_recv, d_send, d_recv,
    load_sem, small_sem, as_sem, ar_sem, bs_sem, br_sem, p0s_sem, p0r_sem, c1s_sem, c1r_sem, c2s_sem, c2r_sem, ds_sem, dr_sem,
):
    me_d = lax.axis_index("dp")
    me_c = lax.axis_index("chan")
    core = lax.rem(me_d, 2)
    me_g = lax.div(me_d, 2)
    groups = n_dp // 2
    chunks = x_v.shape[1] // NB
    hid = w1_hbm.shape[1]
    half = hid // 2
    tiles = NB // 2
    span = NB * LANES

    def chan_peer(j):
        return lax.rem(me_c + j, n_chan)

    def dp_peer(j):
        return lax.rem(me_d + j, n_dp)

    def remote(src, dst, ssem, rsem, dp, chan):
        return pltpu.make_async_remote_copy(
            src_ref=src, dst_ref=dst, send_sem=ssem, recv_sem=rsem,
            device_id={"dp": dp, "chan": chan}, device_id_type=pl.DeviceIdType.MESH,
        )

    barrier = pltpu.get_barrier_semaphore()
    for j in range(1, n_chan):
        pl.semaphore_signal(barrier, inc=1, device_id={"dp": me_d, "chan": chan_peer(j)}, device_id_type=pl.DeviceIdType.MESH)
    for j in range(1, n_dp):
        pl.semaphore_signal(barrier, inc=1, device_id={"dp": dp_peer(j), "chan": me_c}, device_id_type=pl.DeviceIdType.MESH)

    def load(which, src, dst, part):
        lo = part * 64
        rows = pl.ds(lo, 64 if part < 2 else patches - lo)
        return pltpu.make_async_copy(src.at[rows], dst.at[rows], load_sem.at[which, part])

    for part in range(3):
        load(0, x_hbm, x_v, part).start()
    small = [
        pltpu.make_async_copy(src, dst, small_sem.at[i])
        for i, (src, dst) in enumerate(
            ((w1_hbm, w1_ref), (w2_hbm, w2_ref), (bf_hbm, bf_ref), (gain_hbm, gain_ref), (bias_hbm, bias_ref))
        )
    ]
    for copy in small:
        copy.start()
    for part in range(3):
        load(1, u_hbm, u_v, part).start()

    blocks = -(-patches // 8)
    second_row = -(-blocks // 8) * 8
    eye = lax.broadcasted_iota(jnp.int32, (LANES, LANES), 0) == lax.broadcasted_iota(jnp.int32, (LANES, LANES), 1)

    def dense(value):
        n = value.shape[0]
        return jnp.sum(jnp.where(eye[:n], value, 0.0), axis=0, keepdims=True)

    def spread(row):
        return jnp.broadcast_to(row, (LANES, LANES)).T

    def over_blocks(body, init, lo=0, hi=None, unroll=4):
        hi = blocks if hi is None else hi
        whole = min(hi, patches // 8) - lo

        def step(i, carry):
            for k in range(unroll):
                carry = body(lo + i * unroll + k, LANES, carry)
            return carry

        carry = lax.fori_loop(0, whole // unroll, step, init)
        for k in range(whole // unroll * unroll, whole):
            carry = body(lo + k, LANES, carry)
        if hi > patches // 8:
            carry = body(hi - 1, (patches % 8) * NB, carry)
        return carry

    def images_of(ref, g, n, ch):
        return ref[pl.ds(g * 8, n // NB), pl.ds(ch * NB, NB), :].reshape(n, LANES)

    ones = jnp.ones((LANES, LANES), BF16)
    for part in range(3):
        load(0, x_hbm, x_v, part).wait()

        def stat(g, n, carry):
            for ch in range(chunks):
                v = images_of(x_v, g, n, ch)
                total = jnp.dot(v, ones, preferred_element_type=F32)
                v = v.astype(F32)
                a_send[ch, pl.ds(g, 1), :] = dense(total)
                squares = jnp.broadcast_to(jnp.sum(v * v, axis=-1, keepdims=True), (n, LANES))
                a_send[ch, pl.ds(second_row + g, 1), :] = dense(squares)
            return carry

        over_blocks(stat, 0, part * 8, part * 8 + 8 if part < 2 else None, US)
    pl.semaphore_wait(barrier, n_chan - 1 + n_dp - 1)
    for ch in range(chunks):
        for j in range(1, n_chan):
            remote(a_send.at[ch], a_recv.at[ch, j], as_sem.at[ch, j], ar_sem.at[ch, j], me_d, chan_peer(j)).start()

    def select(lo, count):
        at = lo + lax.broadcasted_iota(jnp.int32, (count, hid), 0)
        h, rest_ = at // half, at % half
        unit = rest_ // 8 * 16 + h * 8 + rest_ % 8
        return jnp.where(lax.broadcasted_iota(jnp.int32, (count, hid), 1) == unit, 1.0, 0.0).astype(BF16)

    for copy in small:
        copy.wait()
    tail = patches // 16 * 16
    left = patches - tail
    for ref, dst in ((w1_ref, w1f), (w2_ref, w2f)):
        dst[pl.ds(0, tail), :] = ref[pl.ds(0, tail), :]
        wtail[...] = jnp.zeros((16, hid), F32)
        wtail[pl.ds(0, left), :] = ref[pl.ds(tail, left), :].astype(F32)
        if ref is w1_ref:
            rem = bf_ref[...]
            for i in range(3):
                piece = rem.astype(BF16).astype(F32)
                wtail[pl.ds(left + i, 1), :] = piece
                rem = rem - piece
        dst[pl.ds(tail, 16), :] = wtail[...].astype(BF16)
    for h in range(2):
        pick = select(h * half, half)
        rows = pl.ds(h * half, half)
        w1a[rows, :] = contract_lanes(pick, w1f[...]).astype(BF16)
        w2t[rows, :] = contract_lanes(pick, w2f[...]).astype(BF16)
        w1t[:, rows] = contract_lanes(w1f[pl.ds(0, patches), :], pick).astype(BF16)

    tmp[...] = jnp.zeros_like(tmp)
    def ungroup(g, ch, dst, fill):
        for b in range(NB):
            v = tmp[pl.ds(b, 16, stride=NB), :]
            if fill is not None:
                v = fill(v)
            at = pl.multiple_of(ch * span + b * LANES, LANES)
            rows = pl.ds(pl.multiple_of(g * 16, 16), 16)
            dst[rows, pl.ds(at, LANES)] = v.astype(BF16)

    full = patches // 16
    rest = patches - full * 16
    sub = lax.broadcasted_iota(jnp.int32, (16, LANES), 0)

    for part in range(3):
        load(1, u_hbm, u_v, part).wait()
    for ch in range(chunks):

        def up_group(g, _, ch=ch):
            tmp[...] = u_v[pl.ds(g * 16, 16), pl.ds(ch * NB, NB), :].reshape(16 * NB, LANES).astype(F32)
            ungroup(g, ch, up, None)
            return 0

        lax.fori_loop(0, full, up_group, 0)
        tmp[pl.ds(0, rest * NB), :] = images_of(u_v, full * 2, rest * NB, ch).astype(F32)
        ungroup(full, ch, up, lambda v: jnp.where(sub < rest, v, 0.0))

    def ga_tile(n, _):
        at = pl.ds(pl.multiple_of(n * 256, 256), 256)
        ga[:, at] = jnp.dot(w2t[...], up[:, at], preferred_element_type=F32).astype(BF16)
        return 0

    lax.fori_loop(0, chunks * tiles, ga_tile, 0, unroll=UG)

    owned_b = []

    gain = gain_ref[...]
    bias = bias_ref[...]

    def received(send, recv, ssem, rsem, ch):
        for j in range(1, n_chan):
            remote(send.at[ch], recv.at[ch, j], ssem.at[ch, j], rsem.at[ch, j], me_d, chan_peer(j)).wait_recv()
        totals = []
        for lo in (0, second_row):
            total = send[ch, pl.ds(lo, blocks), :]
            for j in range(1, n_chan):
                total = total + recv[ch, j, pl.ds(lo, blocks), :]
            totals.append(total)
        return totals

    def normalise(ch):
        total, squares = received(a_send, a_recv, as_sem, ar_sem, ch)
        mean = total / width
        mean_d[ch] = mean
        inv_d[ch] = lax.rsqrt(squares / width - mean * mean + EPS)

        def block(g, n):
            m = spread(mean_d[ch, pl.ds(g, 1), :])[:n]
            inv = spread(inv_d[ch, pl.ds(g, 1), :])[:n]
            rows = pl.ds(pl.multiple_of(g * LANES, 64), n)
            normed = (images_of(x_v, g, n, ch).astype(F32) - m) * inv
            normed_n[ch, rows, :] = normed
            inv_n[ch, rows, :] = inv
            return normed * gain + bias

        def pair(g, carry):
            for k in range(2):
                tmp[pl.ds(k * LANES, LANES), :] = block(g * 2 + k, LANES)
            ungroup(g, ch, mx, None)
            return carry

        lax.fori_loop(0, full, pair, 0, unroll=UN)
        tmp[pl.ds(0, rest * NB), :] = block(blocks - 1, rest * NB)
        ungroup(full, ch, mx, lambda v: jnp.where(sub < rest, v, jnp.where(sub < rest + 3, 1.0, 0.0)))

    def hidden(h, ch):
        rows = pl.ds(h * half, half)

        def tile(n, _):
            at = pl.ds(pl.multiple_of(ch * span + n * 256, 256), 256)
            pre = jnp.dot(w1a[rows, :], mx[:, at], preferred_element_type=F32)
            t = pre * 0.7071067811865476
            cdf = 0.5 * lax.erf(t) + 0.5
            act[:, pl.ds(pl.multiple_of(n * 256, 256), 256)] = (pre * cdf).astype(BF16)
            slope = cdf + (t * 0.5641895835477563) * jnp.exp(-(t * t))
            gp[rows, at] = (ga[rows, at].astype(F32) * slope).astype(BF16)
            return 0

        lax.fori_loop(0, tiles, tile, 0, unroll=UH)
        at = pl.ds(ch * span, span)
        first = contract_lanes(gp[rows, at], mx[:, at]).reshape(groups, 2, -1, PP)
        second = contract_lanes(act[...], up[:, at]).reshape(groups, 2, -1, PP)
        if ch:
            first = first + acc[h, :, :, :, pl.ds(0, PP)]
            second = second + acc[h, :, :, :, pl.ds(256, PP)]
        acc[h, :, :, :, pl.ds(0, PP)] = first
        acc[h, :, :, :, pl.ds(256, PP)] = second

    def p0(h):
        return remote(acc.at[h, :, 1 - core], p0_recv.at[h], p0s_sem.at[h], p0r_sem.at[h], me_d + 1 - 2 * core, me_c)

    def c1(h, j):
        g = lax.rem(me_g + j, groups)
        return remote(csum.at[h, g], c1_recv.at[h, me_g], c1s_sem.at[h, j], c1r_sem.at[h, me_g], 2 * g + core, me_c)

    def c1_arrival(h, j):
        g = lax.rem(me_g + j, groups)
        return remote(csum.at[h, g], c1_recv.at[h, g], c1s_sem.at[h, j], c1r_sem.at[h, g], 2 * g + core, me_c)

    def c2(h, j):
        return remote(c1_sum.at[h], c2_recv.at[h, me_c], c2s_sem.at[h, j], c2r_sem.at[h, me_c], me_d, chan_peer(j))

    def c2_arrival(h, j):
        c = chan_peer(j)
        return remote(c1_sum.at[h], c2_recv.at[h, c], c2s_sem.at[h, j], c2r_sem.at[h, c], me_d, c)

    def pair_done(h):
        p0(h).wait()
        csum[h] = acc[h, :, core] + p0_recv[h]
        for j in range(1, groups):
            c1(h, j).start()

    def group_done(h):
        c1_recv[h, me_g] = csum[h, me_g]
        for j in range(1, groups):
            c1_arrival(h, j).wait_recv()
        total = c1_recv[h, 0]
        for g in range(1, groups):
            total = total + c1_recv[h, g]
        c1_sum[h] = total
        c2_recv[h, me_c] = total
        for j in range(1, n_chan):
            c2(h, j).start()

    def all_done(h):
        for j in range(1, n_chan):
            c2_arrival(h, j).wait_recv()
        total = c2_recv[h, 0]
        for c in range(1, n_chan):
            total = total + c2_recv[h, c]
        total = total * scale
        first_ref[pl.ds(h * 8, 8), :] = total[:, :patches]
        here = lax.broadcasted_iota(jnp.int32, (8, LANES), 0) + h * 8 == lax.broadcasted_iota(jnp.int32, (8, LANES), 1)
        owned_b.append(jnp.sum(jnp.where(here, total[:, patches : patches + 1], 0.0), axis=0, keepdims=True))
        second_ref[pl.ds(h * 8, 8), :] = total[:, 256 : 256 + patches]

    wide = lax.broadcasted_iota(jnp.int32, (16, 256), 0) == lax.broadcasted_iota(jnp.int32, (16, 256), 1) // LANES
    both_ones = jnp.where(wide, 1.0, 0.0).astype(BF16)

    def back(ch):
        for n in range(tiles):
            at = pl.ds(pl.multiple_of(ch * span + n * 256, 256), 256)
            gm = jnp.dot(w1t[...], gp[:, at], preferred_element_type=F32)
            for i in range(2):
                gm_n[ch, pl.ds(n * 2 + i, patches, stride=NB), :] = gm[:, i * LANES : (i + 1) * LANES]

    def row_sums(ch, grads):
        def sums(g, n, carry):
            dg, ds = carry
            rows = pl.ds(pl.multiple_of(g * LANES, 64), n)
            gm = gm_n[ch, rows, :]
            normed = normed_n[ch, rows, :]
            both = gm * normed
            gn = gm * gain
            gm_n[ch, rows, :] = gn * inv_n[ch, rows, :]
            pair = jnp.concatenate([gn.astype(BF16), (both * gain).astype(BF16)], axis=1)
            total = contract_lanes(both_ones, pair)
            b_send[ch, pl.ds(g, 1), :n] = total[0:1]
            b_send[ch, pl.ds(second_row + g, 1), :n] = total[1:2]
            return dg + both.reshape(-1, 8, LANES).sum(axis=0), ds + gm.reshape(-1, 8, LANES).sum(axis=0)

        grads = over_blocks(sums, grads, unroll=UR)
        for j in range(1, n_chan):
            remote(b_send.at[ch], b_recv.at[ch, j], bs_sem.at[ch, j], br_sem.at[ch, j], me_d, chan_peer(j)).start()
        return grads

    grads = (jnp.zeros((8, LANES), F32),) * 2
    for ch in range(chunks):
        normalise(ch)
    for ch in range(chunks):
        hidden(0, ch)
    p0(0).start()
    for ch in range(chunks):
        hidden(1, ch)
        if ch == 0:
            pair_done(0)
            back(0)
            grads = row_sums(0, grads)
    p0(1).start()

    for ch in range(1, chunks):
        back(ch)
        if ch == 1:
            pair_done(1)
        grads = row_sums(ch, grads)

    mine = jnp.concatenate([jnp.sum(v, axis=0, keepdims=True) for v in grads], axis=0)
    d_send[...] = mine
    d_recv[me_d] = mine
    for j in range(1, n_dp):
        remote(d_send, d_recv.at[me_d], ds_sem.at[j], dr_sem.at[me_d], dp_peer(j), me_c).start()

    for ch in range(chunks):
        if ch == 1:
            group_done(0)
        if ch == chunks - 1:
            group_done(1)
        totals = received(b_send, b_recv, bs_sem, br_sem, ch)
        for dst, total in zip((first_d, second_d), totals):
            dst[...] = total * inv_d[ch] / width

        def finish(g, n, carry, ch=ch):
            rows = pl.ds(pl.multiple_of(g * LANES, 64), n)
            f = spread(first_d[pl.ds(g, 1), :])[:n]
            q = spread(second_d[pl.ds(g, 1), :])[:n]
            v = images_of(u_v, g, n, ch).astype(F32) + gm_n[ch, rows, :] - f - q * normed_n[ch, rows, :]
            out_ref[pl.ds(g * 8, n // NB), pl.ds(ch * NB, NB), :] = v.astype(BF16).reshape(n // NB, NB, LANES)
            return carry

        over_blocks(finish, 0, unroll=UF)

    all_done(0)
    for j in range(1, n_dp):
        d = dp_peer(j)
        remote(d_send, d_recv.at[d], ds_sem.at[j], dr_sem.at[d], d, me_c).wait_recv()
    vec = d_recv[0]
    for d in range(1, n_dp):
        vec = vec + d_recv[d]
    gain_g_ref[...] = vec[0:1] * scale
    shift_g_ref[...] = vec[1:2] * scale
    all_done(1)
    first_b_ref[...] = (owned_b[0] + owned_b[1])[:, :16]

    for ch in range(chunks):
        for j in range(1, n_chan):
            remote(a_send.at[ch], a_recv.at[ch, j], as_sem.at[ch, j], ar_sem.at[ch, j], me_d, chan_peer(j)).wait_send()
            remote(b_send.at[ch], b_recv.at[ch, j], bs_sem.at[ch, j], br_sem.at[ch, j], me_d, chan_peer(j)).wait_send()
    for h in range(2):
        for j in range(1, groups):
            c1(h, j).wait_send()
        for j in range(1, n_chan):
            c2(h, j).wait_send()
    for j in range(1, n_dp):
        remote(d_send, d_recv.at[me_d], ds_sem.at[j], dr_sem.at[me_d], dp_peer(j), me_c).wait_send()


def per_device(n_dp, n_chan, inputs, norm_gain, norm_bias, w_first, b_first, w_second, upstream):
    images, patches, local = inputs.shape
    hid = w_first.shape[0]
    groups = n_dp // 2
    chunks = images // NB
    width = float(local * n_chan)
    scale = 1.0 / (images * n_dp)
    rows = hid // (groups * 4)
    blocks = -(-patches // 8)
    stat_rows = -(-blocks // 8) * 8 + blocks
    stat = (chunks, stat_rows, LANES)
    vmem = pl.BlockSpec(memory_space=pltpu.VMEM)
    hbm = pl.BlockSpec(memory_space=pltpu.HBM)
    dma = pltpu.SemaphoreType.DMA
    out, first, second, first_b, gain_g, shift_g = pl.pallas_call(
        functools.partial(kernel, n_dp, n_chan, patches, width, scale),
        out_shape=(
            jax.ShapeDtypeStruct((patches, images, local), BF16),
            jax.ShapeDtypeStruct((2 * rows, patches), F32),
            jax.ShapeDtypeStruct((2 * rows, patches), F32),
            jax.ShapeDtypeStruct((1, 2 * rows), F32),
            jax.ShapeDtypeStruct((1, local), F32),
            jax.ShapeDtypeStruct((1, local), F32),
        ),
        in_specs=[hbm] * 7,
        out_specs=(vmem,) * 6,
        scratch_shapes=[
            pltpu.VMEM((1, local), F32),
            pltpu.VMEM((1, local), F32),
            pltpu.VMEM((patches, hid), BF16),
            pltpu.VMEM((1, hid), F32),
            pltpu.VMEM((patches, hid), BF16),
            pltpu.VMEM((PP, hid), BF16),
            pltpu.VMEM((PP, hid), BF16),
            pltpu.VMEM((16, hid), F32),
            pltpu.VMEM((hid, PP), BF16),
            pltpu.VMEM((patches, hid), BF16),
            pltpu.VMEM((hid, PP), BF16),
            pltpu.VMEM((patches, images, local), BF16),
            pltpu.VMEM((patches, images, local), BF16),
            pltpu.VMEM((PP, images * local), BF16),
            pltpu.VMEM((PP, images * local), BF16),
            pltpu.VMEM((hid, images * local), BF16),
            pltpu.VMEM((hid, images * local), BF16),
            pltpu.VMEM((hid // 2, NB * local), BF16),
            pltpu.VMEM((chunks, patches * NB, local), F32),
            pltpu.VMEM((chunks, patches * NB, local), F32),
            pltpu.VMEM((chunks, patches * NB, local), F32),
            pltpu.VMEM((16 * NB, local), F32),
            pltpu.VMEM((chunks, blocks, LANES), F32),
            pltpu.VMEM((chunks, blocks, LANES), F32),
            pltpu.VMEM((blocks, LANES), F32),
            pltpu.VMEM((blocks, LANES), F32),
            pltpu.VMEM((2, groups, 2, rows, 4 * LANES), F32),
            pltpu.VMEM(stat, F32),
            pltpu.VMEM((chunks, n_chan, stat_rows, LANES), F32),
            pltpu.VMEM(stat, F32),
            pltpu.VMEM((chunks, n_chan, stat_rows, LANES), F32),
            pltpu.VMEM((2, groups, rows, 4 * LANES), F32),
            pltpu.VMEM((2, groups, rows, 4 * LANES), F32),
            pltpu.VMEM((2, groups, rows, 4 * LANES), F32),
            pltpu.VMEM((2, rows, 4 * LANES), F32),
            pltpu.VMEM((2, n_chan, rows, 4 * LANES), F32),
            pltpu.VMEM((2, local), F32),
            pltpu.VMEM((n_dp, 2, local), F32),
            dma((2, 3)),
            dma((5,)),
            dma((chunks, n_chan)),
            dma((chunks, n_chan)),
            dma((chunks, n_chan)),
            dma((chunks, n_chan)),
            dma((2,)),
            dma((2,)),
            dma((2, groups)),
            dma((2, groups)),
            dma((2, n_chan)),
            dma((2, n_chan)),
            dma((n_dp,)),
            dma((n_dp,)),
        ],
        compiler_params=pltpu.CompilerParams(
            collective_id=0, has_side_effects=True, vmem_limit_bytes=VMEM_LIMIT
        ),
    )(
        pltpu.with_memory_space_constraint(inputs.transpose(1, 0, 2), pltpu.HBM),
        pltpu.with_memory_space_constraint(upstream.transpose(1, 0, 2), pltpu.HBM),
        pltpu.with_memory_space_constraint(norm_gain.reshape(1, local), pltpu.HBM),
        pltpu.with_memory_space_constraint(norm_bias.reshape(1, local), pltpu.HBM),
        pltpu.with_memory_space_constraint(w_first.T, pltpu.HBM),
        pltpu.with_memory_space_constraint(b_first.reshape(1, hid), pltpu.HBM),
        pltpu.with_memory_space_constraint(w_second, pltpu.HBM),
    )
    return (
        out.transpose(1, 0, 2),
        first,
        second.T,
        first_b[0],
        gain_g[0],
        shift_g[0],
    )


def solution(mesh):
    in_specs = (P("dp", None, "chan"), P("chan"), P("chan"), P(), P(), P(), P("dp", None, "chan"))
    out_specs = (P("dp", None, "chan"), P("dp", None), P(None, "dp"), P("dp"), P("chan"), P("chan"))
    body = functools.partial(per_device, mesh.shape["dp"], mesh.shape["chan"])
    return jax.shard_map(
        body, mesh=mesh, in_specs=in_specs, out_specs=out_specs, check_vma=False
    )
```

```python
import functools

import jax
import jax.numpy as jnp
from jax import lax
from jax.experimental import pallas as pl
from jax.experimental.pallas import tpu as pltpu
from jax.sharding import PartitionSpec as P

EPS = 1e-06
NB = 16
PP = 208
LANES = 128
UG = 8
US = 4
UN = 6
UR = 8
UF = 8
VMEM_LIMIT = 51_500_000
UH = 8
F32 = jnp.float32
BF16 = jnp.bfloat16


def contract_lanes(a, b):
    return lax.dot_general(a, b, (((1,), (1,)), ((), ())), preferred_element_type=F32)


def kernel(
    n_dp, n_chan, patches, width, scale,
    x_hbm, u_hbm, gain_hbm, bias_hbm, w1_hbm, bf_hbm, w2_hbm,
    out_ref, owned_ref, vec_ref,
    gain_ref, bias_ref, w1_ref, bf_ref, w2_ref, w1f, w2f, wtail, w1a, w1t, w2t,
    x_v, u_v, mx, up, ga, gp, act, normed_n, inv_n, gm_n, tmp, mean_d, inv_d, first_d, second_d, acc,
    a_send, a_recv, b_send, b_recv, p0_recv, csum, c1_recv, c1_sum, c2_recv, d_send, d_recv,
    load_sem, small_sem, as_sem, ar_sem, bs_sem, br_sem, p0s_sem, p0r_sem, c1s_sem, c1r_sem, c2s_sem, c2r_sem, ds_sem, dr_sem,
):
    me_d = lax.axis_index("dp")
    me_c = lax.axis_index("chan")
    core = lax.rem(me_d, 2)
    me_g = lax.div(me_d, 2)
    groups = n_dp // 2
    chunks = x_v.shape[1] // NB
    hid = w1_hbm.shape[1]
    half = hid // 2
    tiles = NB // 2
    span = NB * LANES

    def chan_peer(j):
        return lax.rem(me_c + j, n_chan)

    def dp_peer(j):
        return lax.rem(me_d + j, n_dp)

    def remote(src, dst, ssem, rsem, dp, chan):
        return pltpu.make_async_remote_copy(
            src_ref=src, dst_ref=dst, send_sem=ssem, recv_sem=rsem,
            device_id={"dp": dp, "chan": chan}, device_id_type=pl.DeviceIdType.MESH,
        )

    far_groups = sorted(range(1, groups), key=lambda j: -min(j, groups - j))
    far_dp = sorted(range(1, n_dp), key=lambda j: -min(j, n_dp - j))
    turn = n_chan // 2
    far_chan = sorted(range(1, n_chan), key=lambda j: (-min(j % turn, turn - j % turn), -j))

    barrier = pltpu.get_barrier_semaphore()
    for j in range(1, n_chan):
        pl.semaphore_signal(barrier, inc=1, device_id={"dp": me_d, "chan": chan_peer(j)}, device_id_type=pl.DeviceIdType.MESH)
    for j in range(1, n_dp):
        pl.semaphore_signal(barrier, inc=1, device_id={"dp": dp_peer(j), "chan": me_c}, device_id_type=pl.DeviceIdType.MESH)

    def load(which, src, dst, part):
        lo = part * 64
        rows = pl.ds(lo, 64 if part < 2 else patches - lo)
        return pltpu.make_async_copy(src.at[rows], dst.at[rows], load_sem.at[which, part])

    for part in range(3):
        load(0, x_hbm, x_v, part).start()
    small = [
        pltpu.make_async_copy(src, dst, small_sem.at[i])
        for i, (src, dst) in enumerate(
            ((w1_hbm, w1_ref), (w2_hbm, w2_ref), (bf_hbm, bf_ref), (gain_hbm, gain_ref), (bias_hbm, bias_ref))
        )
    ]
    for copy in small:
        copy.start()
    for part in range(3):
        load(1, u_hbm, u_v, part).start()

    blocks = -(-patches // 8)
    second_row = blocks
    eye = lax.broadcasted_iota(jnp.int32, (LANES, LANES), 0) == lax.broadcasted_iota(jnp.int32, (LANES, LANES), 1)

    def dense(value):
        n = value.shape[0]
        return jnp.sum(jnp.where(eye[:n], value, 0.0), axis=0, keepdims=True)

    def spread(row):
        return jnp.broadcast_to(row, (LANES, LANES)).T

    def over_blocks(body, init, lo=0, hi=None, unroll=4):
        hi = blocks if hi is None else hi
        whole = min(hi, patches // 8) - lo

        def step(i, carry):
            for k in range(unroll):
                carry = body(lo + i * unroll + k, LANES, carry)
            return carry

        carry = lax.fori_loop(0, whole // unroll, step, init)
        for k in range(whole // unroll * unroll, whole):
            carry = body(lo + k, LANES, carry)
        if hi > patches // 8:
            carry = body(hi - 1, (patches % 8) * NB, carry)
        return carry

    def images_of(ref, g, n, ch):
        return ref[pl.ds(g * 8, n // NB), pl.ds(ch * NB, NB), :].reshape(n, LANES)

    ones = jnp.ones((LANES, LANES), BF16)
    for part in range(3):
        load(0, x_hbm, x_v, part).wait()

        def stat(g, n, carry):
            for ch in range(chunks):
                v = images_of(x_v, g, n, ch)
                total = jnp.dot(v, ones, preferred_element_type=F32)
                v = v.astype(F32)
                a_send[ch, pl.ds(g, 1), :] = dense(total)
                squares = jnp.broadcast_to(jnp.sum(v * v, axis=-1, keepdims=True), (n, LANES))
                a_send[ch, pl.ds(second_row + g, 1), :] = dense(squares)
            return carry

        over_blocks(stat, 0, part * 8, part * 8 + 8 if part < 2 else None, US)
    pl.semaphore_wait(barrier, n_chan - 1 + n_dp - 1)
    for ch in range(chunks):
        for j in far_chan:
            remote(a_send.at[ch], a_recv.at[ch, j], as_sem.at[ch, j], ar_sem.at[ch, j], me_d, chan_peer(j)).start()

    def select(lo, count):
        at = lo + lax.broadcasted_iota(jnp.int32, (count, hid), 0)
        h, rest_ = at // half, at % half
        unit = rest_ // 8 * 16 + h * 8 + rest_ % 8
        return jnp.where(lax.broadcasted_iota(jnp.int32, (count, hid), 1) == unit, 1.0, 0.0).astype(BF16)

    for copy in small:
        copy.wait()
    tail = patches // 16 * 16
    left = patches - tail
    for ref, dst in ((w1_ref, w1f), (w2_ref, w2f)):
        dst[pl.ds(0, tail), :] = ref[pl.ds(0, tail), :]
        wtail[...] = jnp.zeros((16, hid), F32)
        wtail[pl.ds(0, left), :] = ref[pl.ds(tail, left), :].astype(F32)
        if ref is w1_ref:
            rem = bf_ref[...]
            for i in range(3):
                piece = rem.astype(BF16).astype(F32)
                wtail[pl.ds(left + i, 1), :] = piece
                rem = rem - piece
        dst[pl.ds(tail, 16), :] = wtail[...].astype(BF16)
    for h in range(2):
        pick = select(h * half, half)
        rows = pl.ds(h * half, half)
        w1a[rows, :] = contract_lanes(pick, w1f[...]).astype(BF16)
        w2t[rows, :] = contract_lanes(pick, w2f[...]).astype(BF16)
        w1t[:, rows] = contract_lanes(w1f[pl.ds(0, patches), :], pick).astype(BF16)

    tmp[...] = jnp.zeros_like(tmp)
    def ungroup(g, ch, dst, fill):
        for b in range(NB):
            v = tmp[pl.ds(b, 16, stride=NB), :]
            if fill is not None:
                v = fill(v)
            at = pl.multiple_of(ch * span + b * LANES, LANES)
            rows = pl.ds(pl.multiple_of(g * 16, 16), 16)
            dst[rows, pl.ds(at, LANES)] = v.astype(BF16)

    full = patches // 16
    rest = patches - full * 16
    sub = lax.broadcasted_iota(jnp.int32, (16, LANES), 0)

    for part in range(3):
        load(1, u_hbm, u_v, part).wait()
    for ch in range(chunks):

        def up_group(g, _, ch=ch):
            tmp[...] = u_v[pl.ds(g * 16, 16), pl.ds(ch * NB, NB), :].reshape(16 * NB, LANES).astype(F32)
            ungroup(g, ch, up, None)
            return 0

        lax.fori_loop(0, full, up_group, 0)
        tmp[pl.ds(0, rest * NB), :] = images_of(u_v, full * 2, rest * NB, ch).astype(F32)
        ungroup(full, ch, up, lambda v: jnp.where(sub < rest, v, 0.0))

    def ga_tile(n, _):
        at = pl.ds(pl.multiple_of(n * 256, 256), 256)
        ga[:, at] = jnp.dot(w2t[...], up[:, at], preferred_element_type=F32).astype(BF16)
        return 0

    lax.fori_loop(0, chunks * tiles, ga_tile, 0, unroll=UG)

    owned_b = []

    gain = gain_ref[...]
    bias = bias_ref[...]

    def received(send, recv, ssem, rsem, ch):
        for j in range(1, n_chan):
            remote(send.at[ch], recv.at[ch, j], ssem.at[ch, j], rsem.at[ch, j], me_d, chan_peer(j)).wait_recv()
        totals = []
        for lo in (0, second_row):
            total = send[ch, pl.ds(lo, blocks), :]
            for j in range(1, n_chan):
                total = total + recv[ch, j, pl.ds(lo, blocks), :]
            totals.append(total)
        return totals

    def normalise(ch):
        total, squares = received(a_send, a_recv, as_sem, ar_sem, ch)
        mean = total / width
        mean_d[ch] = mean
        inv_d[ch] = lax.rsqrt(squares / width - mean * mean + EPS)

        def block(g, n):
            m = spread(mean_d[ch, pl.ds(g, 1), :])[:n]
            inv = spread(inv_d[ch, pl.ds(g, 1), :])[:n]
            rows = pl.ds(pl.multiple_of(g * LANES, 64), n)
            normed = (images_of(x_v, g, n, ch).astype(F32) - m) * inv
            normed_n[ch, rows, :] = normed
            inv_n[ch, rows, :] = inv
            return normed * gain + bias

        def pair(g, carry):
            for k in range(2):
                tmp[pl.ds(k * LANES, LANES), :] = block(g * 2 + k, LANES)
            ungroup(g, ch, mx, None)
            return carry

        lax.fori_loop(0, full, pair, 0, unroll=UN)
        tmp[pl.ds(0, rest * NB), :] = block(blocks - 1, rest * NB)
        ungroup(full, ch, mx, lambda v: jnp.where(sub < rest, v, jnp.where(sub < rest + 3, 1.0, 0.0)))

    def hidden(h, ch):
        rows = pl.ds(h * half, half)

        def tile(n, _):
            at = pl.ds(pl.multiple_of(ch * span + n * 256, 256), 256)
            pre = jnp.dot(w1a[rows, :], mx[:, at], preferred_element_type=F32)
            t = pre * 0.7071067811865476
            cdf = 0.5 * lax.erf(t) + 0.5
            act[:, pl.ds(pl.multiple_of(n * 256, 256), 256)] = (pre * cdf).astype(BF16)
            slope = cdf + (t * 0.5641895835477563) * jnp.exp2((t * t) * -1.4426950408889634)
            gp[rows, at] = (ga[rows, at].astype(F32) * slope).astype(BF16)
            return 0

        lax.fori_loop(0, tiles, tile, 0, unroll=UH)
        at = pl.ds(ch * span, span)
        first = contract_lanes(gp[rows, at], mx[:, at]).reshape(groups, 2, -1, PP)
        second = contract_lanes(act[...], up[:, at]).reshape(groups, 2, -1, PP)
        if ch:
            first = first + acc[h, :, :, :, pl.ds(0, PP)]
            second = second + acc[h, :, :, :, pl.ds(256, PP)]
        acc[h, :, :, :, pl.ds(0, PP)] = first
        acc[h, :, :, :, pl.ds(256, PP)] = second

    def p0(h):
        return remote(acc.at[h, :, 1 - core], p0_recv.at[h], p0s_sem.at[h], p0r_sem.at[h], me_d + 1 - 2 * core, me_c)

    def c1(h, j):
        g = lax.rem(me_g + j, groups)
        return remote(csum.at[h, g], c1_recv.at[h, me_g], c1s_sem.at[h, j], c1r_sem.at[h, me_g], 2 * g + core, me_c)

    def c1_arrival(h, j):
        g = lax.rem(me_g + j, groups)
        return remote(csum.at[h, g], c1_recv.at[h, g], c1s_sem.at[h, j], c1r_sem.at[h, g], 2 * g + core, me_c)

    def c2(h, j):
        return remote(c1_sum.at[h], c2_recv.at[h, me_c], c2s_sem.at[h, j], c2r_sem.at[h, me_c], me_d, chan_peer(j))

    def c2_arrival(h, j):
        c = chan_peer(j)
        return remote(c1_sum.at[h], c2_recv.at[h, c], c2s_sem.at[h, j], c2r_sem.at[h, c], me_d, c)

    def pair_done(h):
        p0(h).wait()
        csum[h] = acc[h, :, core] + p0_recv[h]
        for j in far_groups:
            c1(h, j).start()

    def group_done(h):
        c1_recv[h, me_g] = csum[h, me_g]
        for j in range(1, groups):
            c1_arrival(h, j).wait_recv()
        total = c1_recv[h, 0]
        for g in range(1, groups):
            total = total + c1_recv[h, g]
        c1_sum[h] = total
        c2_recv[h, me_c] = total
        for j in far_chan:
            c2(h, j).start()

    def all_done(h):
        for j in range(1, n_chan):
            c2_arrival(h, j).wait_recv()
        total = c2_recv[h, 0]
        for c in range(1, n_chan):
            total = total + c2_recv[h, c]
        total = total * scale
        owned_ref[0, pl.ds(h * 8, 8), :] = total[:, :patches]
        here = lax.broadcasted_iota(jnp.int32, (8, LANES), 0) + h * 8 == lax.broadcasted_iota(jnp.int32, (8, LANES), 1)
        owned_b.append(jnp.sum(jnp.where(here, total[:, patches : patches + 1], 0.0), axis=0, keepdims=True))
        owned_ref[1, pl.ds(h * 8, 8), :] = total[:, 256 : 256 + patches]

    wide = lax.broadcasted_iota(jnp.int32, (16, 256), 0) == lax.broadcasted_iota(jnp.int32, (16, 256), 1) // LANES
    both_ones = jnp.where(wide, 1.0, 0.0).astype(BF16)

    def back(ch):
        for n in range(tiles):
            at = pl.ds(pl.multiple_of(ch * span + n * 256, 256), 256)
            gm = jnp.dot(w1t[...], gp[:, at], preferred_element_type=F32)
            for i in range(2):
                gm_n[ch, pl.ds(n * 2 + i, patches, stride=NB), :] = gm[:, i * LANES : (i + 1) * LANES]

    def row_sums(ch, grads):
        def sums(g, n, carry):
            dg, ds = carry
            rows = pl.ds(pl.multiple_of(g * LANES, 64), n)
            gm = gm_n[ch, rows, :]
            normed = normed_n[ch, rows, :]
            both = gm * normed
            gn = gm * gain
            gm_n[ch, rows, :] = gn * inv_n[ch, rows, :]
            pair = jnp.concatenate([gn.astype(BF16), (both * gain).astype(BF16)], axis=1)
            total = contract_lanes(both_ones, pair)
            b_send[ch, pl.ds(g, 1), :n] = total[0:1]
            b_send[ch, pl.ds(second_row + g, 1), :n] = total[1:2]
            return dg + both.reshape(-1, 8, LANES).sum(axis=0), ds + gm.reshape(-1, 8, LANES).sum(axis=0)

        grads = over_blocks(sums, grads, unroll=UR)
        for j in far_chan:
            remote(b_send.at[ch], b_recv.at[ch, j], bs_sem.at[ch, j], br_sem.at[ch, j], me_d, chan_peer(j)).start()
        return grads

    grads = (jnp.zeros((8, LANES), F32),) * 2
    for ch in range(chunks):
        normalise(ch)
    for ch in range(chunks):
        hidden(0, ch)
    p0(0).start()
    for ch in range(chunks):
        hidden(1, ch)
        if ch == 0:
            pair_done(0)
            back(0)
            grads = row_sums(0, grads)
    p0(1).start()

    for ch in range(1, chunks):
        back(ch)
        if ch == 1:
            pair_done(1)
        grads = row_sums(ch, grads)

    mine = jnp.concatenate([jnp.sum(v, axis=0, keepdims=True) for v in grads], axis=0)
    d_send[...] = mine
    d_recv[me_d] = mine
    for j in far_dp:
        remote(d_send, d_recv.at[me_d], ds_sem.at[j], dr_sem.at[me_d], dp_peer(j), me_c).start()

    for ch in range(chunks):
        if ch == 1:
            group_done(0)
        if ch == chunks - 1:
            group_done(1)
        totals = received(b_send, b_recv, bs_sem, br_sem, ch)
        for dst, total in zip((first_d, second_d), totals):
            dst[...] = total * inv_d[ch] / width

        def finish(g, n, carry, ch=ch):
            rows = pl.ds(pl.multiple_of(g * LANES, 64), n)
            f = spread(first_d[pl.ds(g, 1), :])[:n]
            q = spread(second_d[pl.ds(g, 1), :])[:n]
            v = images_of(u_v, g, n, ch).astype(F32) + gm_n[ch, rows, :] - f - q * normed_n[ch, rows, :]
            out_ref[pl.ds(g * 8, n // NB), pl.ds(ch * NB, NB), :] = v.astype(BF16).reshape(n // NB, NB, LANES)
            return carry

        over_blocks(finish, 0, unroll=UF)

    all_done(0)
    for j in range(1, n_dp):
        d = dp_peer(j)
        remote(d_send, d_recv.at[d], ds_sem.at[j], dr_sem.at[d], d, me_c).wait_recv()
    vec = d_recv[0]
    for d in range(1, n_dp):
        vec = vec + d_recv[d]
    vec_ref[pl.ds(0, 2), :] = vec * scale
    all_done(1)
    vec_ref[pl.ds(2, 1), :] = owned_b[0] + owned_b[1]

    for ch in range(chunks):
        for j in range(1, n_chan):
            remote(a_send.at[ch], a_recv.at[ch, j], as_sem.at[ch, j], ar_sem.at[ch, j], me_d, chan_peer(j)).wait_send()
            remote(b_send.at[ch], b_recv.at[ch, j], bs_sem.at[ch, j], br_sem.at[ch, j], me_d, chan_peer(j)).wait_send()
    for h in range(2):
        for j in range(1, groups):
            c1(h, j).wait_send()
        for j in range(1, n_chan):
            c2(h, j).wait_send()
    for j in range(1, n_dp):
        remote(d_send, d_recv.at[me_d], ds_sem.at[j], dr_sem.at[me_d], dp_peer(j), me_c).wait_send()


def per_device(n_dp, n_chan, inputs, norm_gain, norm_bias, w_first, b_first, w_second, upstream):
    images, patches, local = inputs.shape
    hid = w_first.shape[0]
    groups = n_dp // 2
    chunks = images // NB
    width = float(local * n_chan)
    scale = 1.0 / (images * n_dp)
    rows = hid // (groups * 4)
    blocks = -(-patches // 8)
    stat_rows = 2 * blocks
    stat = (chunks, stat_rows, LANES)
    vmem = pl.BlockSpec(memory_space=pltpu.VMEM)
    hbm = pl.BlockSpec(memory_space=pltpu.HBM)
    dma = pltpu.SemaphoreType.DMA
    out, owned, vec = pl.pallas_call(
        functools.partial(kernel, n_dp, n_chan, patches, width, scale),
        out_shape=(
            jax.ShapeDtypeStruct((patches, images, local), BF16),
            jax.ShapeDtypeStruct((2, 2 * rows, patches), F32),
            jax.ShapeDtypeStruct((3, local), F32),
        ),
        in_specs=[hbm] * 7,
        out_specs=(vmem,) * 3,
        scratch_shapes=[
            pltpu.VMEM((1, local), F32),
            pltpu.VMEM((1, local), F32),
            pltpu.VMEM((patches, hid), BF16),
            pltpu.VMEM((1, hid), F32),
            pltpu.VMEM((patches, hid), BF16),
            pltpu.VMEM((PP, hid), BF16),
            pltpu.VMEM((PP, hid), BF16),
            pltpu.VMEM((16, hid), F32),
            pltpu.VMEM((hid, PP), BF16),
            pltpu.VMEM((patches, hid), BF16),
            pltpu.VMEM((hid, PP), BF16),
            pltpu.VMEM((patches, images, local), BF16),
            pltpu.VMEM((patches, images, local), BF16),
            pltpu.VMEM((PP, images * local), BF16),
            pltpu.VMEM((PP, images * local), BF16),
            pltpu.VMEM((hid, images * local), BF16),
            pltpu.VMEM((hid, images * local), BF16),
            pltpu.VMEM((hid // 2, NB * local), BF16),
            pltpu.VMEM((chunks, patches * NB, local), F32),
            pltpu.VMEM((chunks, patches * NB, local), F32),
            pltpu.VMEM((chunks, patches * NB, local), F32),
            pltpu.VMEM((16 * NB, local), F32),
            pltpu.VMEM((chunks, blocks, LANES), F32),
            pltpu.VMEM((chunks, blocks, LANES), F32),
            pltpu.VMEM((blocks, LANES), F32),
            pltpu.VMEM((blocks, LANES), F32),
            pltpu.VMEM((2, groups, 2, rows, 4 * LANES), F32),
            pltpu.VMEM(stat, F32),
            pltpu.VMEM((chunks, n_chan, stat_rows, LANES), F32),
            pltpu.VMEM(stat, F32),
            pltpu.VMEM((chunks, n_chan, stat_rows, LANES), F32),
            pltpu.VMEM((2, groups, rows, 4 * LANES), F32),
            pltpu.VMEM((2, groups, rows, 4 * LANES), F32),
            pltpu.VMEM((2, groups, rows, 4 * LANES), F32),
            pltpu.VMEM((2, rows, 4 * LANES), F32),
            pltpu.VMEM((2, n_chan, rows, 4 * LANES), F32),
            pltpu.VMEM((2, local), F32),
            pltpu.VMEM((n_dp, 2, local), F32),
            dma((2, 3)),
            dma((5,)),
            dma((chunks, n_chan)),
            dma((chunks, n_chan)),
            dma((chunks, n_chan)),
            dma((chunks, n_chan)),
            dma((2,)),
            dma((2,)),
            dma((2, groups)),
            dma((2, groups)),
            dma((2, n_chan)),
            dma((2, n_chan)),
            dma((n_dp,)),
            dma((n_dp,)),
        ],
        compiler_params=pltpu.CompilerParams(
            collective_id=0, has_side_effects=True, vmem_limit_bytes=VMEM_LIMIT
        ),
    )(
        pltpu.with_memory_space_constraint(inputs.transpose(1, 0, 2), pltpu.HBM),
        pltpu.with_memory_space_constraint(upstream.transpose(1, 0, 2), pltpu.HBM),
        pltpu.with_memory_space_constraint(norm_gain.reshape(1, local), pltpu.HBM),
        pltpu.with_memory_space_constraint(norm_bias.reshape(1, local), pltpu.HBM),
        pltpu.with_memory_space_constraint(w_first.T, pltpu.HBM),
        pltpu.with_memory_space_constraint(b_first.reshape(1, hid), pltpu.HBM),
        pltpu.with_memory_space_constraint(w_second, pltpu.HBM),
    )
    return (
        out.transpose(1, 0, 2),
        owned[0],
        owned[1].T,
        vec[2, : 2 * rows],
        vec[0],
        vec[1],
    )


def solution(mesh):
    in_specs = (P("dp", None, "chan"), P("chan"), P("chan"), P(), P(), P(), P("dp", None, "chan"))
    out_specs = (P("dp", None, "chan"), P("dp", None), P(None, "dp"), P("dp"), P("chan"), P("chan"))
    body = functools.partial(per_device, mesh.shape["dp"], mesh.shape["chan"])
    return jax.shard_map(
        body, mesh=mesh, in_specs=in_specs, out_specs=out_specs, check_vma=False
    )
```

```python
import functools

import jax
import jax.numpy as jnp
from jax import lax
from jax.experimental import pallas as pl
from jax.experimental.pallas import tpu as pltpu
from jax.sharding import PartitionSpec as P

EPS = 1e-06
NB = 16
PP = 208
LANES = 128
UG = 8
US = 4
UN = 6
UR = 8
UF = 8
VMEM_LIMIT = 51_500_000
UH = 8
F32 = jnp.float32
BF16 = jnp.bfloat16


def contract_lanes(a, b):
    return lax.dot_general(a, b, (((1,), (1,)), ((), ())), preferred_element_type=F32)


def kernel(
    n_dp, n_chan, patches, width, scale,
    x_hbm, u_hbm, gain_hbm, bias_hbm, w1_hbm, bf_hbm, w2_hbm,
    out_ref, owned_ref, vec_ref,
    gain_ref, bias_ref, w1_ref, bf_ref, w2_ref, w1f, w2f, wtail, w1a, w1t, w2t,
    x_v, u_v, mx, up, ga, gp, act, normed_n, inv_n, gm_n, tmp, mean_d, inv_d, first_d, second_d, acc,
    a_send, a_recv, b_send, b_recv, p0_recv, csum, c1_recv, c1_sum, c2_recv, d_send, d_recv,
    load_sem, small_sem, as_sem, ar_sem, bs_sem, br_sem, p0s_sem, p0r_sem, c1s_sem, c1r_sem, c2s_sem, c2r_sem, ds_sem, dr_sem,
):
    me_d = lax.axis_index("dp")
    me_c = lax.axis_index("chan")
    core = lax.rem(me_d, 2)
    me_g = lax.div(me_d, 2)
    groups = n_dp // 2
    chunks = x_v.shape[1] // NB
    hid = w1_hbm.shape[1]
    half = hid // 2
    tiles = NB // 2
    span = NB * LANES

    def chan_peer(j):
        return lax.rem(me_c + j, n_chan)

    def dp_peer(j):
        return lax.rem(me_d + j, n_dp)

    def remote(src, dst, ssem, rsem, dp, chan):
        return pltpu.make_async_remote_copy(
            src_ref=src, dst_ref=dst, send_sem=ssem, recv_sem=rsem,
            device_id={"dp": dp, "chan": chan}, device_id_type=pl.DeviceIdType.MESH,
        )

    far_groups = sorted(range(1, groups), key=lambda j: -min(j, groups - j))
    far_dp = sorted(range(1, n_dp), key=lambda j: -min(j, n_dp - j))
    turn = n_chan // 2
    far_chan = sorted(range(1, n_chan), key=lambda j: (-min(j % turn, turn - j % turn), -j))

    barrier = pltpu.get_barrier_semaphore()
    for j in range(1, n_chan):
        pl.semaphore_signal(barrier, inc=1, device_id={"dp": me_d, "chan": chan_peer(j)}, device_id_type=pl.DeviceIdType.MESH)
    for j in range(1, n_dp):
        pl.semaphore_signal(barrier, inc=1, device_id={"dp": dp_peer(j), "chan": me_c}, device_id_type=pl.DeviceIdType.MESH)

    def load(which, src, dst, part):
        lo = part * 64
        rows = pl.ds(lo, 64 if part < 2 else patches - lo)
        return pltpu.make_async_copy(src.at[rows], dst.at[rows], load_sem.at[which, part])

    for part in range(3):
        load(0, x_hbm, x_v, part).start()
    small = [
        pltpu.make_async_copy(src, dst, small_sem.at[i])
        for i, (src, dst) in enumerate(
            ((w1_hbm, w1_ref), (w2_hbm, w2_ref), (bf_hbm, bf_ref), (gain_hbm, gain_ref), (bias_hbm, bias_ref))
        )
    ]
    for copy in small:
        copy.start()
    for part in range(3):
        load(1, u_hbm, u_v, part).start()

    blocks = -(-patches // 8)
    second_row = blocks
    eye = lax.broadcasted_iota(jnp.int32, (LANES, LANES), 0) == lax.broadcasted_iota(jnp.int32, (LANES, LANES), 1)

    def dense(value):
        n = value.shape[0]
        return jnp.sum(jnp.where(eye[:n], value, 0.0), axis=0, keepdims=True)

    def spread(row):
        return jnp.broadcast_to(row, (LANES, LANES)).T

    def over_blocks(body, init, lo=0, hi=None, unroll=4):
        hi = blocks if hi is None else hi
        whole = min(hi, patches // 8) - lo

        def step(i, carry):
            for k in range(unroll):
                carry = body(lo + i * unroll + k, LANES, carry)
            return carry

        carry = lax.fori_loop(0, whole // unroll, step, init)
        for k in range(whole // unroll * unroll, whole):
            carry = body(lo + k, LANES, carry)
        if hi > patches // 8:
            carry = body(hi - 1, (patches % 8) * NB, carry)
        return carry

    def images_of(ref, g, n, ch):
        return ref[pl.ds(g * 8, n // NB), pl.ds(ch * NB, NB), :].reshape(n, LANES)

    ones = jnp.ones((LANES, LANES), BF16)
    for part in range(3):
        load(0, x_hbm, x_v, part).wait()

        def stat(g, n, carry):
            for ch in range(chunks):
                v = images_of(x_v, g, n, ch)
                total = jnp.dot(v, ones, preferred_element_type=F32)
                v = v.astype(F32)
                a_send[ch, pl.ds(g, 1), :] = dense(total)
                squares = jnp.broadcast_to(jnp.sum(v * v, axis=-1, keepdims=True), (n, LANES))
                a_send[ch, pl.ds(second_row + g, 1), :] = dense(squares)
            return carry

        over_blocks(stat, 0, part * 8, part * 8 + 8 if part < 2 else None, US)
    pl.semaphore_wait(barrier, n_chan - 1 + n_dp - 1)
    for ch in range(chunks):
        for j in far_chan:
            remote(a_send.at[ch], a_recv.at[ch, j], as_sem.at[ch, j], ar_sem.at[ch, j], me_d, chan_peer(j)).start()

    def select(lo, count):
        at = lo + lax.broadcasted_iota(jnp.int32, (count, hid), 0)
        h, rest_ = at // half, at % half
        unit = rest_ // 8 * 16 + h * 8 + rest_ % 8
        return jnp.where(lax.broadcasted_iota(jnp.int32, (count, hid), 1) == unit, 1.0, 0.0).astype(BF16)

    for copy in small:
        copy.wait()
    tail = patches // 16 * 16
    left = patches - tail
    for ref, dst in ((w1_ref, w1f), (w2_ref, w2f)):
        dst[pl.ds(0, tail), :] = ref[pl.ds(0, tail), :]
        wtail[...] = jnp.zeros((16, hid), F32)
        wtail[pl.ds(0, left), :] = ref[pl.ds(tail, left), :].astype(F32)
        if ref is w1_ref:
            rem = bf_ref[...]
            for i in range(3):
                piece = rem.astype(BF16).astype(F32)
                wtail[pl.ds(left + i, 1), :] = piece
                rem = rem - piece
        dst[pl.ds(tail, 16), :] = wtail[...].astype(BF16)
    for h in range(2):
        pick = select(h * half, half)
        rows = pl.ds(h * half, half)
        w1a[rows, :] = contract_lanes(pick, w1f[...]).astype(BF16)
        w2t[rows, :] = contract_lanes(pick, w2f[...]).astype(BF16)
        w1t[:, rows] = contract_lanes(w1f[pl.ds(0, patches), :], pick).astype(BF16)

    tmp[...] = jnp.zeros_like(tmp)
    def ungroup(g, ch, dst, fill):
        for b in range(NB):
            v = tmp[pl.ds(b, 16, stride=NB), :]
            if fill is not None:
                v = fill(v)
            at = pl.multiple_of(ch * span + b * LANES, LANES)
            rows = pl.ds(pl.multiple_of(g * 16, 16), 16)
            dst[rows, pl.ds(at, LANES)] = v.astype(BF16)

    full = patches // 16
    rest = patches - full * 16
    sub = lax.broadcasted_iota(jnp.int32, (16, LANES), 0)

    for part in range(3):
        load(1, u_hbm, u_v, part).wait()
    for ch in range(chunks):

        def up_group(g, _, ch=ch):
            tmp[...] = u_v[pl.ds(g * 16, 16), pl.ds(ch * NB, NB), :].reshape(16 * NB, LANES).astype(F32)
            ungroup(g, ch, up, None)
            return 0

        lax.fori_loop(0, full, up_group, 0)
        tmp[pl.ds(0, rest * NB), :] = images_of(u_v, full * 2, rest * NB, ch).astype(F32)
        ungroup(full, ch, up, lambda v: jnp.where(sub < rest, v, 0.0))

    def ga_tile(n, _):
        at = pl.ds(pl.multiple_of(n * 256, 256), 256)
        ga[:, at] = jnp.dot(w2t[...], up[:, at], preferred_element_type=F32).astype(BF16)
        return 0

    lax.fori_loop(0, chunks * tiles, ga_tile, 0, unroll=UG)

    owned_b = []

    gain = gain_ref[...]
    bias = bias_ref[...]

    def received(send, recv, ssem, rsem, ch):
        for j in range(1, n_chan):
            remote(send.at[ch], recv.at[ch, j], ssem.at[ch, j], rsem.at[ch, j], me_d, chan_peer(j)).wait_recv()
        totals = []
        for lo in (0, second_row):
            total = send[ch, pl.ds(lo, blocks), :]
            for j in range(1, n_chan):
                total = total + recv[ch, j, pl.ds(lo, blocks), :]
            totals.append(total)
        return totals

    def normalise(ch):
        total, squares = received(a_send, a_recv, as_sem, ar_sem, ch)
        mean = total / width
        mean_d[ch] = mean
        inv_d[ch] = lax.rsqrt(squares / width - mean * mean + EPS)

        def block(g, n):
            m = spread(mean_d[ch, pl.ds(g, 1), :])[:n]
            inv = spread(inv_d[ch, pl.ds(g, 1), :])[:n]
            rows = pl.ds(pl.multiple_of(g * LANES, 64), n)
            normed = (images_of(x_v, g, n, ch).astype(F32) - m) * inv
            normed_n[ch, rows, :] = normed
            inv_n[ch, rows, :] = inv
            return normed * gain + bias

        def pair(g, carry):
            for k in range(2):
                tmp[pl.ds(k * LANES, LANES), :] = block(g * 2 + k, LANES)
            ungroup(g, ch, mx, None)
            return carry

        lax.fori_loop(0, full, pair, 0, unroll=UN)
        tmp[pl.ds(0, rest * NB), :] = block(blocks - 1, rest * NB)
        ungroup(full, ch, mx, lambda v: jnp.where(sub < rest, v, jnp.where(sub < rest + 3, 1.0, 0.0)))

    def hidden(h, ch):
        rows = pl.ds(h * half, half)

        def tile(n, _):
            at = pl.ds(pl.multiple_of(ch * span + n * 256, 256), 256)
            pre = jnp.dot(w1a[rows, :], mx[:, at], preferred_element_type=F32)
            t = pre * 0.7071067811865476
            cdf = 0.5 * lax.erf(t) + 0.5
            act[:, pl.ds(pl.multiple_of(n * 256, 256), 256)] = (pre * cdf).astype(BF16)
            slope = cdf + (t * 0.5641895835477563) * jnp.exp2((t * t) * -1.4426950408889634)
            gp[rows, at] = (ga[rows, at].astype(F32) * slope).astype(BF16)
            return 0

        lax.fori_loop(0, tiles, tile, 0, unroll=UH)
        at = pl.ds(ch * span, span)
        first = contract_lanes(gp[rows, at], mx[:, at]).reshape(groups, 2, -1, PP)
        second = contract_lanes(act[...], up[:, at]).reshape(groups, 2, -1, PP)
        if ch:
            first = first + acc[h, :, :, :, pl.ds(0, PP)]
            second = second + acc[h, :, :, :, pl.ds(256, PP)]
        acc[h, :, :, :, pl.ds(0, PP)] = first
        acc[h, :, :, :, pl.ds(256, PP)] = second

    def p0(h):
        return remote(acc.at[h, :, 1 - core], p0_recv.at[h], p0s_sem.at[h], p0r_sem.at[h], me_d + 1 - 2 * core, me_c)

    def c1(h, j):
        g = lax.rem(me_g + j, groups)
        return remote(csum.at[h, g], c1_recv.at[h, me_g], c1s_sem.at[h, j], c1r_sem.at[h, me_g], 2 * g + core, me_c)

    def c1_arrival(h, j):
        g = lax.rem(me_g + j, groups)
        return remote(csum.at[h, g], c1_recv.at[h, g], c1s_sem.at[h, j], c1r_sem.at[h, g], 2 * g + core, me_c)

    def c2(h, j):
        return remote(c1_sum.at[h], c2_recv.at[h, me_c], c2s_sem.at[h, j], c2r_sem.at[h, me_c], me_d, chan_peer(j))

    def c2_arrival(h, j):
        c = chan_peer(j)
        return remote(c1_sum.at[h], c2_recv.at[h, c], c2s_sem.at[h, j], c2r_sem.at[h, c], me_d, c)

    def pair_done(h):
        p0(h).wait()
        csum[h] = acc[h, :, core] + p0_recv[h]
        for j in far_groups:
            c1(h, j).start()

    def group_done(h):
        c1_recv[h, me_g] = csum[h, me_g]
        for j in range(1, groups):
            c1_arrival(h, j).wait_recv()
        total = c1_recv[h, 0]
        for g in range(1, groups):
            total = total + c1_recv[h, g]
        c1_sum[h] = total
        c2_recv[h, me_c] = total
        for j in far_chan:
            c2(h, j).start()

    def all_done(h):
        for j in range(1, n_chan):
            c2_arrival(h, j).wait_recv()
        total = c2_recv[h, 0]
        for c in range(1, n_chan):
            total = total + c2_recv[h, c]
        total = total * scale
        owned_ref[0, pl.ds(h * 8, 8), :] = total[:, :patches]
        here = lax.broadcasted_iota(jnp.int32, (8, LANES), 0) + h * 8 == lax.broadcasted_iota(jnp.int32, (8, LANES), 1)
        owned_b.append(jnp.sum(jnp.where(here, total[:, patches : patches + 1], 0.0), axis=0, keepdims=True))
        owned_ref[1, pl.ds(h * 8, 8), :] = total[:, 256 : 256 + patches]

    wide = lax.broadcasted_iota(jnp.int32, (16, 256), 0) == lax.broadcasted_iota(jnp.int32, (16, 256), 1) // LANES
    both_ones = jnp.where(wide, 1.0, 0.0).astype(BF16)

    def back(ch):
        for n in range(tiles):
            at = pl.ds(pl.multiple_of(ch * span + n * 256, 256), 256)
            gm = jnp.dot(w1t[...], gp[:, at], preferred_element_type=F32)
            for i in range(2):
                gm_n[ch, pl.ds(n * 2 + i, patches, stride=NB), :] = gm[:, i * LANES : (i + 1) * LANES]

    def row_sums(ch, grads):
        def sums(g, n, carry):
            dg, ds = carry
            rows = pl.ds(pl.multiple_of(g * LANES, 64), n)
            gm = gm_n[ch, rows, :]
            normed = normed_n[ch, rows, :]
            both = gm * normed
            gn = gm * gain
            gm_n[ch, rows, :] = gn * inv_n[ch, rows, :]
            pair = jnp.concatenate([gn.astype(BF16), (both * gain).astype(BF16)], axis=1)
            total = contract_lanes(both_ones, pair)
            b_send[ch, pl.ds(g, 1), :n] = total[0:1]
            b_send[ch, pl.ds(second_row + g, 1), :n] = total[1:2]
            return dg + both.reshape(-1, 8, LANES).sum(axis=0), ds + gm.reshape(-1, 8, LANES).sum(axis=0)

        grads = over_blocks(sums, grads, unroll=UR)
        for j in far_chan:
            remote(b_send.at[ch], b_recv.at[ch, j], bs_sem.at[ch, j], br_sem.at[ch, j], me_d, chan_peer(j)).start()
        return grads

    grads = (jnp.zeros((8, LANES), F32),) * 2
    for ch in range(chunks):
        normalise(ch)
    for ch in range(chunks):
        hidden(0, ch)
    p0(0).start()
    for ch in range(chunks):
        hidden(1, ch)
        if ch == 0:
            pair_done(0)
            back(0)
    p0(1).start()
    grads = row_sums(0, grads)
    pair_done(1)

    for ch in range(1, chunks):
        back(ch)
        grads = row_sums(ch, grads)

    mine = jnp.concatenate([jnp.sum(v, axis=0, keepdims=True) for v in grads], axis=0)
    d_send[...] = mine
    d_recv[me_d] = mine
    for j in far_dp:
        remote(d_send, d_recv.at[me_d], ds_sem.at[j], dr_sem.at[me_d], dp_peer(j), me_c).start()

    for ch in range(chunks):
        if ch == 1:
            group_done(0)
        if ch == chunks - 1:
            group_done(1)
        totals = received(b_send, b_recv, bs_sem, br_sem, ch)
        for dst, total in zip((first_d, second_d), totals):
            dst[...] = total * inv_d[ch] / width

        def finish(g, n, carry, ch=ch):
            rows = pl.ds(pl.multiple_of(g * LANES, 64), n)
            f = spread(first_d[pl.ds(g, 1), :])[:n]
            q = spread(second_d[pl.ds(g, 1), :])[:n]
            v = images_of(u_v, g, n, ch).astype(F32) + gm_n[ch, rows, :] - f - q * normed_n[ch, rows, :]
            out_ref[pl.ds(g * 8, n // NB), pl.ds(ch * NB, NB), :] = v.astype(BF16).reshape(n // NB, NB, LANES)
            return carry

        over_blocks(finish, 0, unroll=UF)

    all_done(0)
    for j in range(1, n_dp):
        d = dp_peer(j)
        remote(d_send, d_recv.at[d], ds_sem.at[j], dr_sem.at[d], d, me_c).wait_recv()
    vec = d_recv[0]
    for d in range(1, n_dp):
        vec = vec + d_recv[d]
    vec_ref[pl.ds(0, 2), :] = vec * scale
    all_done(1)
    vec_ref[pl.ds(2, 1), :] = owned_b[0] + owned_b[1]

    for ch in range(chunks):
        for j in range(1, n_chan):
            remote(a_send.at[ch], a_recv.at[ch, j], as_sem.at[ch, j], ar_sem.at[ch, j], me_d, chan_peer(j)).wait_send()
            remote(b_send.at[ch], b_recv.at[ch, j], bs_sem.at[ch, j], br_sem.at[ch, j], me_d, chan_peer(j)).wait_send()
    for h in range(2):
        for j in range(1, groups):
            c1(h, j).wait_send()
        for j in range(1, n_chan):
            c2(h, j).wait_send()
    for j in range(1, n_dp):
        remote(d_send, d_recv.at[me_d], ds_sem.at[j], dr_sem.at[me_d], dp_peer(j), me_c).wait_send()


def per_device(n_dp, n_chan, inputs, norm_gain, norm_bias, w_first, b_first, w_second, upstream):
    images, patches, local = inputs.shape
    hid = w_first.shape[0]
    groups = n_dp // 2
    chunks = images // NB
    width = float(local * n_chan)
    scale = 1.0 / (images * n_dp)
    rows = hid // (groups * 4)
    blocks = -(-patches // 8)
    stat_rows = 2 * blocks
    stat = (chunks, stat_rows, LANES)
    vmem = pl.BlockSpec(memory_space=pltpu.VMEM)
    hbm = pl.BlockSpec(memory_space=pltpu.HBM)
    dma = pltpu.SemaphoreType.DMA
    out, owned, vec = pl.pallas_call(
        functools.partial(kernel, n_dp, n_chan, patches, width, scale),
        out_shape=(
            jax.ShapeDtypeStruct((patches, images, local), BF16),
            jax.ShapeDtypeStruct((2, 2 * rows, patches), F32),
            jax.ShapeDtypeStruct((3, local), F32),
        ),
        in_specs=[hbm] * 7,
        out_specs=(vmem,) * 3,
        scratch_shapes=[
            pltpu.VMEM((1, local), F32),
            pltpu.VMEM((1, local), F32),
            pltpu.VMEM((patches, hid), BF16),
            pltpu.VMEM((1, hid), F32),
            pltpu.VMEM((patches, hid), BF16),
            pltpu.VMEM((PP, hid), BF16),
            pltpu.VMEM((PP, hid), BF16),
            pltpu.VMEM((16, hid), F32),
            pltpu.VMEM((hid, PP), BF16),
            pltpu.VMEM((patches, hid), BF16),
            pltpu.VMEM((hid, PP), BF16),
            pltpu.VMEM((patches, images, local), BF16),
            pltpu.VMEM((patches, images, local), BF16),
            pltpu.VMEM((PP, images * local), BF16),
            pltpu.VMEM((PP, images * local), BF16),
            pltpu.VMEM((hid, images * local), BF16),
            pltpu.VMEM((hid, images * local), BF16),
            pltpu.VMEM((hid // 2, NB * local), BF16),
            pltpu.VMEM((chunks, patches * NB, local), F32),
            pltpu.VMEM((chunks, patches * NB, local), F32),
            pltpu.VMEM((chunks, patches * NB, local), F32),
            pltpu.VMEM((16 * NB, local), F32),
            pltpu.VMEM((chunks, blocks, LANES), F32),
            pltpu.VMEM((chunks, blocks, LANES), F32),
            pltpu.VMEM((blocks, LANES), F32),
            pltpu.VMEM((blocks, LANES), F32),
            pltpu.VMEM((2, groups, 2, rows, 4 * LANES), F32),
            pltpu.VMEM(stat, F32),
            pltpu.VMEM((chunks, n_chan, stat_rows, LANES), F32),
            pltpu.VMEM(stat, F32),
            pltpu.VMEM((chunks, n_chan, stat_rows, LANES), F32),
            pltpu.VMEM((2, groups, rows, 4 * LANES), F32),
            pltpu.VMEM((2, groups, rows, 4 * LANES), F32),
            pltpu.VMEM((2, groups, rows, 4 * LANES), F32),
            pltpu.VMEM((2, rows, 4 * LANES), F32),
            pltpu.VMEM((2, n_chan, rows, 4 * LANES), F32),
            pltpu.VMEM((2, local), F32),
            pltpu.VMEM((n_dp, 2, local), F32),
            dma((2, 3)),
            dma((5,)),
            dma((chunks, n_chan)),
            dma((chunks, n_chan)),
            dma((chunks, n_chan)),
            dma((chunks, n_chan)),
            dma((2,)),
            dma((2,)),
            dma((2, groups)),
            dma((2, groups)),
            dma((2, n_chan)),
            dma((2, n_chan)),
            dma((n_dp,)),
            dma((n_dp,)),
        ],
        compiler_params=pltpu.CompilerParams(
            collective_id=0, has_side_effects=True, vmem_limit_bytes=VMEM_LIMIT
        ),
    )(
        pltpu.with_memory_space_constraint(inputs.transpose(1, 0, 2), pltpu.HBM),
        pltpu.with_memory_space_constraint(upstream.transpose(1, 0, 2), pltpu.HBM),
        pltpu.with_memory_space_constraint(norm_gain.reshape(1, local), pltpu.HBM),
        pltpu.with_memory_space_constraint(norm_bias.reshape(1, local), pltpu.HBM),
        pltpu.with_memory_space_constraint(w_first.T, pltpu.HBM),
        pltpu.with_memory_space_constraint(b_first.reshape(1, hid), pltpu.HBM),
        pltpu.with_memory_space_constraint(w_second, pltpu.HBM),
    )
    return (
        out.transpose(1, 0, 2),
        owned[0],
        owned[1].T,
        vec[2, : 2 * rows],
        vec[0],
        vec[1],
    )


def solution(mesh):
    in_specs = (P("dp", None, "chan"), P("chan"), P("chan"), P(), P(), P(), P("dp", None, "chan"))
    out_specs = (P("dp", None, "chan"), P("dp", None), P(None, "dp"), P("dp"), P("chan"), P("chan"))
    body = functools.partial(per_device, mesh.shape["dp"], mesh.shape["chan"])
    return jax.shard_map(
        body, mesh=mesh, in_specs=in_specs, out_specs=out_specs, check_vma=False
    )
```
